256 devices in a mesh: unit: 4 (over z_lo), lat: 4 (over y), lon: 4 (over x_lo, core), lev: 4 (over z_hi, x_hi).
Axes of the slice: x: 4 (x_hi: 2, x_lo: 2; x = x_hi * 2 + x_lo), y: 4, z: 8 (z_hi: 2, z_lo: 4; z = z_hi * 4 + z_lo), core: 2. Of those that a mesh axis runs over, the one named last changes fastest.
Arguments:
- tracer: float32 [64, 256, 128, 128], P(('unit', 'lat'), 'lon', 'lev'), parts along dimension 0, may hold values from 0.2 to 1.8
- crowding: float32 [64, 256, 128, 128], P(('unit', 'lat'), 'lon', 'lev'), parts along dimension 0, may hold values from 0.5 to 2
Outputs:
- column_sum: float32 [64, 256, 128, 128], P(('unit', 'lat'), 'lon', 'lev'), parts along dimension 0
- tracer_end: float32 [64, 256, 128, 128], P(('unit', 'lat'), 'lon', 'lev'), parts along dimension 0
The draws below stay inside these ranges and needn't reach their ends.
There are 4 independent parts, one for each index of `unit`. The reference program is written for one: setup_inputs(seed, part) draws one part's arguments, and reference() takes and returns one part's arrays. A program takes and returns all parts, laid end to end along the dimension named above; each array names one. Nothing has to cross between parts.
All inputs are finite; a program needn't handle non-finite values.
Results may differ from the reference program's by a relative error of at most 0.00002.
Values sent between devices are 32-bit elements; how exact they have to be, the bound alone decides.
A program may use at most 128 MiB of HBM per device.

```python
import jax
import jax.numpy as jnp
from jax import lax

GRID_J = 16
GRID_I = 256
GRID_K = 128
LEVELS = 128
STEPS = 4


def steps_of(key, extent, pieces, low, top_value):
    level = 1.0
    for axis_at, shards_of in pieces:
        draws = jax.random.uniform(jax.random.fold_in(jax.random.fold_in(key, 6), axis_at), (shards_of,), jnp.float32, low / len(pieces), top_value / len(pieces))
        level = level * jnp.repeat(jnp.exp(draws), extent[axis_at] // shards_of).reshape((-1,) + (1,) * (len(extent) - 1 - axis_at))
    return level


def setup_inputs(seed: int = 0, part: int = 0) -> dict:
    key_of = jax.random.split(jax.random.key(seed), 3)
    part_keys = jax.random.split(jax.random.fold_in(key_of[2], part), 3)
    return {
        "tracer": jnp.clip(0.2 + 1.5999999 * jax.random.uniform(part_keys[0], (GRID_J, GRID_I, GRID_K, LEVELS), jnp.float32) ** steps_of(part_keys[0], (GRID_J, GRID_I, GRID_K, LEVELS), ((0, 4), (1, 4), (2, 4)), -0.2, 0.2), 0.2, 1.8),
        "crowding": jnp.clip(0.5 + 1.5 * jax.random.uniform(part_keys[1], (GRID_J, GRID_I, GRID_K, LEVELS), jnp.float32) ** steps_of(part_keys[1], (GRID_J, GRID_I, GRID_K, LEVELS), ((0, 4), (1, 4), (2, 4)), -0.2, 0.2), 0.5, 2.0),
    }


def without_rim(values, dims):
    for dim in dims:
        values = lax.slice_in_dim(values, 1, values.shape[dim] - 1, axis=dim)
    return values


def shifted_cells(values, dim, start, dims):
    others = [other for other in dims if other != dim]
    values = without_rim(values, others)
    return lax.slice_in_dim(values, start, start + values.shape[dim] - 2, axis=dim)


def march_step(padded, crowding):
    middle = without_rim(padded, (0, 1, 2))
    lower = [shifted_cells(padded, dim, 0, (0, 1, 2)) for dim in (0, 1, 2)]
    upper = [shifted_cells(padded, dim, 2, (0, 1, 2)) for dim in (0, 1, 2)]
    spread = lower[0] + upper[0] + lower[1] + upper[1] + lower[2] + upper[2] - 6.0 * middle
    return middle + 0.1 * spread + 0.2 * middle * (1.0 - middle * crowding)


def reference(tracer, crowding):
    for step in range(STEPS):
        tracer = march_step(jnp.pad(tracer, ((1, 1), (1, 1), (1, 1), (0, 0)), mode="constant"), crowding)
    column_sum = jnp.cumsum(tracer, axis=0) / GRID_J
    return column_sum, tracer
```

```python
import functools

import jax
import jax.numpy as jnp
from jax import lax
from jax.experimental import pallas as pl
from jax.experimental.pallas import tpu as pltpu
from jax.sharding import PartitionSpec as P

STEPS = 4
ROWS = 4
MESH = pl.DeviceIdType.MESH
AXES = ("unit", "lat", "lon", "lev")


def march_kernel(rows, tracer, crowding, end, carried, t, c, faces, edges, total, load_sem, send_sem,
                 lat_sem, lon_sem, lev_sem, carry_sem):
    nj, ni, nk, levels = tracer.shape
    chunks = ni // (2 * rows)
    at = {axis: lax.axis_index(axis) for axis in AXES}
    size = {axis: lax.axis_size(axis) for axis in AXES}

    def has(axis, side):
        return at[axis] > 0 if side == 0 else at[axis] < size[axis] - 1

    def there(axis, side):
        return {axis: at[axis] - 1 if side == 0 else at[axis] + 1}

    def starts(m):
        return (m * rows, ni - (m + 1) * rows)

    def lat_copy(s, a, length, m, side, source=None):
        row = 0 if side == 0 else nj - 1
        if source is None:
            source = t.at[s, 1 + row, pl.ds(1 + a, length)]
        return pltpu.make_async_remote_copy(
            source, t.at[s, nj + 1 if side == 0 else 0, pl.ds(1 + a, length)],
            send_sem.at[side], lat_sem.at[s, m, 1 - side], device_id=there("lat", side), device_id_type=MESH)

    def lon_copy(s, side, source=None):
        if source is None:
            source = t.at[s, pl.ds(1, nj), 1 if side == 0 else ni]
        return pltpu.make_async_remote_copy(
            source, t.at[s, pl.ds(1, nj), ni + 1 if side == 0 else 0],
            send_sem.at[2 + side], lon_sem.at[s, 1 - side], device_id=there("lon", side), device_id_type=MESH)

    def lev_copy(s, a, length, m, side):
        return pltpu.make_async_remote_copy(
            faces.at[s, side, pl.ds(a, length)], edges.at[s, 1 - side, pl.ds(a, length)],
            send_sem.at[4 + side], lev_sem.at[s, m, 1 - side], device_id=there("lev", side), device_id_type=MESH)

    def carry_copy(a, length, n):
        return pltpu.make_async_remote_copy(
            total.at[pl.ds(a, length)], carried.at[pl.ds(a, length)],
            send_sem.at[6], carry_sem.at[n], device_id=there("lat", 1), device_id_type=MESH)

    load_t = pltpu.make_async_copy(tracer, t.at[0, pl.ds(1, nj), pl.ds(1, ni)], load_sem.at[0])
    load_c = pltpu.make_async_copy(crowding, c, load_sem.at[1])

    barrier = pltpu.get_barrier_semaphore()
    for axis in AXES[1:]:
        for side in (0, 1):
            @pl.when(has(axis, side))
            def _():
                pl.semaphore_signal(barrier, inc=1, device_id=there(axis, side), device_id_type=MESH)
    load_t.start()
    load_c.start()

    zero = jnp.zeros((nk, levels), jnp.float32)
    for side in (0, 1):
        @pl.when(jnp.logical_not(has("lat", side)))
        def _():
            @pl.loop(0, ni)
            def _(i):
                for s in range(STEPS):
                    t[s, 0 if side == 0 else nj + 1, 1 + i] = zero

            if side == 0:
                @pl.loop(0, ni)
                def _(i):
                    carried[i] = zero

        @pl.when(jnp.logical_not(has("lon", side)))
        def _():
            for s in range(STEPS):
                for j in range(nj):
                    t[s, 1 + j, 0 if side == 0 else ni + 1] = zero

        @pl.when(jnp.logical_not(has("lev", side)))
        def _():
            @pl.loop(0, ni)
            def _(i):
                for s in range(STEPS):
                    for j in range(nj):
                        edges[s, side, i, j] = jnp.zeros((1, levels), jnp.float32)

    neighbours = sum(
        has(axis, side).astype(jnp.int32) for axis in AXES[1:] for side in (0, 1))
    pl.semaphore_wait(barrier, neighbours)

    for m in range(chunks):
        for side in (0, 1):
            @pl.when(has("lat", side))
            def _():
                for a in starts(m):
                    lat_copy(0, a, rows, m, side,
                             tracer.at[0 if side == 0 else nj - 1, pl.ds(a, rows)]).start()
    for side in (0, 1):
        @pl.when(has("lon", side))
        def _():
            lon_copy(0, side, tracer.at[:, 0 if side == 0 else ni - 1]).start()

    def send_lev(s, m):
        for side in (0, 1):
            @pl.when(has("lev", side))
            def _():
                for a in starts(m):
                    lev_copy(s, a, rows, m, side).start()

    load_t.wait()

    @pl.loop(0, chunks)
    def _(m):
        @pl.loop(0, rows)
        def _(r):
            for a in starts(m):
                for j in range(nj):
                    faces[0, 0, a + r, j] = t[0, 1 + j, 1 + a + r, 0:1]
                    faces[0, 1, a + r, j] = t[0, 1 + j, 1 + a + r, nk - 1:nk]
        send_lev(0, m)

    load_c.wait()

    below = lax.broadcasted_iota(jnp.int32, (nk, levels), 0) == 0
    above = lax.broadcasted_iota(jnp.int32, (nk, levels), 0) == nk - 1

    def stepped(s, i):
        for j in range(nj):
            middle = t[s, 1 + j, 1 + i]
            lower = jnp.where(below, edges[s, 0, i, j], pltpu.roll(middle, 1, 0))
            upper = jnp.where(above, edges[s, 1, i, j], pltpu.roll(middle, nk - 1, 0))
            spread = (t[s, j, 1 + i] + t[s, 2 + j, 1 + i] + t[s, 1 + j, i] + t[s, 1 + j, 2 + i]
                      + lower + upper - 6.0 * middle)
            yield j, middle + 0.1 * spread + 0.2 * middle * (1.0 - middle * c[j, i])

    def arrived(s, m):
        for side in (0, 1):
            @pl.when(has("lat", side))
            def _():
                lat_copy(s, 0, 2 * rows, m, 1 - side).wait_recv()

            @pl.when(has("lev", side))
            def _():
                lev_copy(s, 0, 2 * rows, m, 1 - side).wait_recv()

            @pl.when(jnp.logical_and(has("lon", side), m == 0))
            def _():
                lon_copy(s, 1 - side).wait_recv()

    @pl.loop(0, STEPS - 1)
    def _(s):
        @pl.loop(0, chunks)
        def _(m):
            arrived(s, m)

            @pl.loop(0, rows)
            def _(r):
                for a in starts(m):
                    for j, value in stepped(s, a + r):
                        t[s + 1, 1 + j, 1 + a + r] = value
                        faces[s + 1, 0, a + r, j] = value[0:1]
                        faces[s + 1, 1, a + r, j] = value[nk - 1:nk]

            for side in (0, 1):
                @pl.when(has("lat", side))
                def _():
                    for a in starts(m):
                        lat_copy(s + 1, a, rows, m, side).start()
            send_lev(s + 1, m)
            for side in (0, 1):
                @pl.when(jnp.logical_and(has("lon", side), m == 0))
                def _():
                    lon_copy(s + 1, side).start()

    first = at["lat"] == 0

    @pl.loop(0, chunks)
    def _(m):
        arrived(STEPS - 1, m)

        @pl.loop(0, rows)
        def _(r):
            for a in starts(m):
                summed = None
                for j, value in stepped(STEPS - 1, a + r):
                    end[j, a + r] = value
                    summed = value if j == 0 else summed + value
                total[a + r] = summed

        @pl.when(first)
        def _():
            for n, a in enumerate(starts(m)):
                carry_copy(a, rows, 2 * m + n).start()

    @pl.when(jnp.logical_not(first))
    def _():
        @pl.loop(0, chunks)
        def _(m):
            for n, a in enumerate(starts(m)):
                carry_copy(a, rows, 2 * m + n).wait_recv()

                @pl.when(has("lat", 1))
                def _():
                    @pl.loop(0, rows)
                    def _(r):
                        total[a + r] = total[a + r] + carried[a + r]
                    carry_copy(a, rows, 2 * m + n).start()

    for side in (0, 1):
        @pl.when(has("lat", side))
        def _():
            for s in range(STEPS):
                lat_copy(s, 0, ni, 0, side).wait_send()

        @pl.when(has("lon", side))
        def _():
            for s in range(STEPS):
                lon_copy(s, side).wait_send()

        @pl.when(has("lev", side))
        def _():
            for s in range(STEPS):
                lev_copy(s, 0, ni, 0, side).wait_send()

    @pl.when(has("lat", 1))
    def _():
        carry_copy(0, ni, 0).wait_send()


def march(tracer, crowding, rows):
    nj, ni, nk, levels = tracer.shape
    chunks = ni // (2 * rows)
    f32 = jnp.float32
    dma = pltpu.SemaphoreType.DMA
    return pl.pallas_call(
        functools.partial(march_kernel, rows),
        out_shape=(jax.ShapeDtypeStruct(tracer.shape, f32), jax.ShapeDtypeStruct(tracer.shape[1:], f32)),
        in_specs=[pl.BlockSpec(memory_space=pl.ANY)] * 2,
        out_specs=(pl.BlockSpec(memory_space=pltpu.VMEM),) * 2,
        scratch_shapes=[
            pltpu.VMEM((STEPS, nj + 2, ni + 2, nk, levels), f32),
            pltpu.VMEM((nj, ni, nk, levels), f32),
            pltpu.VMEM((STEPS, 2, ni, nj, 1, levels), f32),
            pltpu.VMEM((STEPS, 2, ni, nj, 1, levels), f32),
            pltpu.VMEM((ni, nk, levels), f32),
            dma((2,)),
            dma((7,)),
            dma((STEPS, chunks, 2)),
            dma((STEPS, 2)),
            dma((STEPS, chunks, 2)),
            dma((2 * chunks,)),
        ],
        compiler_params=pltpu.CompilerParams(
            collective_id=0, has_side_effects=True, vmem_limit_bytes=48 * 2**20),
        name="march",
    )(tracer, crowding)


def sums_kernel(scale, end, carried, sums, copied):
    run = carried[...]
    for j in range(end.shape[0]):
        value = end[j]
        run = run + value
        sums[j] = run * scale
        copied[j] = value


def sums_along_j(end, carried, cells):
    nj, ni, nk, levels = end.shape
    block = min(8, ni)
    whole = pl.BlockSpec((nj, block, nk, levels), lambda i: (0, i, 0, 0))
    return pl.pallas_call(
        functools.partial(sums_kernel, 1.0 / cells),
        grid=(ni // block,),
        out_shape=(jax.ShapeDtypeStruct(end.shape, end.dtype),) * 2,
        in_specs=[whole, pl.BlockSpec((block, nk, levels), lambda i: (i, 0, 0))],
        out_specs=(whole, whole),
        compiler_params=pltpu.CompilerParams(vmem_limit_bytes=12 * 2**20),
        name="sums",
    )(end, carried)


def on_device(tracer, crowding):
    end, carried = march(tracer, crowding, min(ROWS, tracer.shape[1] // 2))
    return sums_along_j(end, carried, tracer.shape[0] * lax.axis_size("lat"))


def solution(mesh):
    spec = P(("unit", "lat"), "lon", "lev", None)
    return jax.shard_map(
        on_device, mesh=mesh, in_specs=(spec, spec), out_specs=(spec, spec), check_vma=False)
```

```python
import functools

import jax
import jax.numpy as jnp
from jax import lax
from jax.experimental import pallas as pl
from jax.experimental.pallas import tpu as pltpu
from jax.sharding import PartitionSpec as P

STEPS = 4
ROWS = 4
AROUND = 6
RETURNED = 3
MESH = pl.DeviceIdType.MESH
AXES = ("unit", "lat", "lon", "lev")


def march_kernel(rows, tracer, crowding, end, carried, t, c, faces, edges, total, suffix, whole,
                 load_sem, send_sem, lat_sem, lon_sem, lev_sem, carry_sem, suffix_sem, whole_sem):
    nj, ni, nk, levels = tracer.shape
    chunks = ni // (2 * rows)
    at = {axis: lax.axis_index(axis) for axis in AXES}
    size = {axis: lax.axis_size(axis) for axis in AXES}

    def has(axis, side):
        return at[axis] > 0 if side == 0 else at[axis] < size[axis] - 1

    def there(axis, side):
        return {axis: at[axis] - 1 if side == 0 else at[axis] + 1}

    def starts(m):
        return (m * rows, ni - (m + 1) * rows)

    def lat_copy(s, a, length, m, side, source=None):
        row = 0 if side == 0 else nj - 1
        if source is None:
            source = t.at[s, 1 + row, pl.ds(1 + a, length)]
        return pltpu.make_async_remote_copy(
            source, t.at[s, nj + 1 if side == 0 else 0, pl.ds(1 + a, length)],
            send_sem.at[side], lat_sem.at[s, m, 1 - side], device_id=there("lat", side), device_id_type=MESH)

    def lon_copy(s, side, source=None):
        if source is None:
            source = t.at[s, pl.ds(1, nj), 1 if side == 0 else ni]
        return pltpu.make_async_remote_copy(
            source, t.at[s, pl.ds(1, nj), ni + 1 if side == 0 else 0],
            send_sem.at[2 + side], lon_sem.at[s, 1 - side], device_id=there("lon", side), device_id_type=MESH)

    def lev_copy(s, a, length, m, side):
        return pltpu.make_async_remote_copy(
            faces.at[s, side, pl.ds(a, length)], edges.at[s, 1 - side, pl.ds(a, length)],
            send_sem.at[4 + side], lev_sem.at[s, m, 1 - side], device_id=there("lev", side), device_id_type=MESH)

    pieces = 2 * chunks
    last = size["lat"] - 1

    def span(p, count=1):
        m = p // 2
        return pl.ds(jnp.where(p % 2 == 0, m * rows, ni - (m + 1) * rows), count * rows)

    def carry_copy(p, count=1):
        at_p = span(p) if count == 1 else pl.ds(0, count * rows)
        return pltpu.make_async_remote_copy(
            total.at[at_p], carried.at[at_p], send_sem.at[6], carry_sem.at[p],
            device_id=there("lat", 1), device_id_type=MESH)

    def suffix_copy(p, source, count=1):
        at_p = span(p) if count == 1 else pl.ds(0, count * rows)
        return pltpu.make_async_remote_copy(
            source.at[at_p], suffix.at[at_p], send_sem.at[7], suffix_sem.at[p],
            device_id=there("lat", 0), device_id_type=MESH)

    def round_copy(p, count=1):
        at_p = span(p) if count == 1 else pl.ds(0, count * rows)
        return pltpu.make_async_remote_copy(
            suffix.at[at_p], carried.at[at_p], send_sem.at[8], carry_sem.at[p],
            device_id={"lat": last}, device_id_type=MESH)

    def whole_copy(p, source, count=1):
        at_p = span(p) if count == 1 else pl.ds(0, count * rows)
        return pltpu.make_async_remote_copy(
            source.at[at_p], whole.at[at_p], send_sem.at[9], whole_sem.at[p],
            device_id=there("lat", 0), device_id_type=MESH)

    load_t = pltpu.make_async_copy(tracer, t.at[0, pl.ds(1, nj), pl.ds(1, ni)], load_sem.at[0])
    load_c = pltpu.make_async_copy(crowding, c, load_sem.at[1])

    barrier = pltpu.get_barrier_semaphore()

    def greet(axis, side, where=None):
        pl.semaphore_signal(
            barrier, inc=1, device_id=there(axis, side) if where is None else where, device_id_type=MESH)

    for axis in ("lat", "lon"):
        for side in (0, 1):
            pl.when(has(axis, side))(functools.partial(greet, axis, side))
    ends = jnp.logical_or(at["lat"] == 0, at["lat"] == last)
    pl.when(ends)(functools.partial(greet, "lat", 0, {"lat": last - at["lat"]}))
    load_t.start()
    load_c.start()

    zero = jnp.zeros((nk, levels), jnp.float32)
    for side in (0, 1):
        @pl.when(jnp.logical_not(has("lat", side)))
        def _():
            @pl.loop(0, ni)
            def _(i):
                for s in range(STEPS):
                    t[s, 0 if side == 0 else nj + 1, 1 + i] = zero

            if side == 0:
                @pl.loop(0, ni)
                def _(i):
                    carried[i] = zero

        @pl.when(jnp.logical_not(has("lon", side)))
        def _():
            for s in range(STEPS):
                for j in range(nj):
                    t[s, 1 + j, 0 if side == 0 else ni + 1] = zero

        @pl.when(jnp.logical_not(has("lev", side)))
        def _():
            @pl.loop(0, ni)
            def _(i):
                for s in range(STEPS):
                    for j in range(nj):
                        edges[s, side, i, j] = jnp.zeros((1, levels), jnp.float32)

    def count(axis):
        return has(axis, 0).astype(jnp.int32) + has(axis, 1).astype(jnp.int32)

    odd = at["lev"] % 2 == 1
    near = count("lat") + count("lon") + ends.astype(jnp.int32)
    pl.semaphore_wait(barrier, near + jnp.where(odd, 0, count("lev")))

    for m in range(chunks):
        for side in (0, 1):
            @pl.when(has("lat", side))
            def _():
                for a in starts(m):
                    lat_copy(0, a, rows, m, side,
                             tracer.at[0 if side == 0 else nj - 1, pl.ds(a, rows)]).start()
    for side in (0, 1):
        @pl.when(has("lon", side))
        def _():
            lon_copy(0, side, tracer.at[:, 0 if side == 0 else ni - 1]).start()

    for side in (0, 1):
        pl.when(has("lev", side))(functools.partial(greet, "lev", side))

    def send_lev(s, m):
        for side in (0, 1):
            @pl.when(has("lev", side))
            def _():
                for a in starts(m):
                    lev_copy(s, a, rows, m, side).start()

    load_t.wait()

    @pl.loop(0, chunks)
    def _(m):
        @pl.loop(0, rows)
        def _(r):
            for a in starts(m):
                for j in range(nj):
                    faces[0, 0, a + r, j] = t[0, 1 + j, 1 + a + r, 0:1]
                    faces[0, 1, a + r, j] = t[0, 1 + j, 1 + a + r, nk - 1:nk]

    @pl.when(odd)
    def _():
        pl.semaphore_wait(barrier, count("lev"))

    @pl.loop(0, chunks)
    def _(m):
        send_lev(0, m)

    load_c.wait()

    below = lax.broadcasted_iota(jnp.int32, (nk, levels), 0) == 0
    above = lax.broadcasted_iota(jnp.int32, (nk, levels), 0) == nk - 1

    def stepped(s, i):
        for j in range(nj):
            middle = t[s, 1 + j, 1 + i]
            lower = jnp.where(below, edges[s, 0, i, j], pltpu.roll(middle, 1, 0))
            upper = jnp.where(above, edges[s, 1, i, j], pltpu.roll(middle, nk - 1, 0))
            spread = (t[s, j, 1 + i] + t[s, 2 + j, 1 + i] + t[s, 1 + j, i] + t[s, 1 + j, 2 + i]
                      + lower + upper - 6.0 * middle)
            yield j, middle + 0.1 * spread + 0.2 * middle * (1.0 - middle * c[j, i])

    def arrived(s, m):
        for side in (0, 1):
            @pl.when(has("lat", side))
            def _():
                lat_copy(s, 0, 2 * rows, m, 1 - side).wait_recv()

            @pl.when(has("lev", side))
            def _():
                lev_copy(s, 0, 2 * rows, m, 1 - side).wait_recv()

            @pl.when(jnp.logical_and(has("lon", side), m == 0))
            def _():
                lon_copy(s, 1 - side).wait_recv()

    @pl.loop(0, STEPS - 1)
    def _(s):
        @pl.loop(0, chunks)
        def _(m):
            arrived(s, m)

            @pl.loop(0, rows)
            def _(r):
                for a in starts(m):
                    for j, value in stepped(s, a + r):
                        t[s + 1, 1 + j, 1 + a + r] = value
                        faces[s + 1, 0, a + r, j] = value[0:1]
                        faces[s + 1, 1, a + r, j] = value[nk - 1:nk]

            for side in (0, 1):
                @pl.when(has("lat", side))
                def _():
                    for a in starts(m):
                        lat_copy(s + 1, a, rows, m, side).start()
            send_lev(s + 1, m)
            for side in (0, 1):
                @pl.when(jnp.logical_and(has("lon", side), m == 0))
                def _():
                    lon_copy(s + 1, side).start()

    def block(n):
        return pl.when(at["lat"] == n)

    @pl.loop(0, chunks)
    def _(m):
        arrived(STEPS - 1, m)

        @pl.loop(0, rows)
        def _(r):
            for a in starts(m):
                summed = None
                for j, value in stepped(STEPS - 1, a + r):
                    end[j, a + r] = value
                    summed = value if j == 0 else summed + value
                total[a + r] = summed

        for p in (2 * m, 2 * m + 1):
            @pl.when(jnp.logical_and(at["lat"] == 0, p >= AROUND))
            def _():
                carry_copy(p).start()

            @pl.when(jnp.logical_and(at["lat"] == last - 1, p < AROUND))
            def _():
                suffix_copy(p, total).start()

    def add_suffix(p):
        suffix_copy(p, suffix).wait_recv()

        @pl.loop(0, rows)
        def _(r):
            i = span(p).start + r
            suffix[i] = suffix[i] + total[i]

    def pass_up(p):
        carry_copy(p).wait_recv()

        @pl.loop(0, rows)
        def _(r):
            i = span(p).start + r
            total[i] = total[i] + carried[i]
        carry_copy(p).start()

    def take_off(p, own):
        @pl.loop(0, rows)
        def _(r):
            i = span(p).start + r
            carried[i] = whole[i] - own[i]

    @block(0)
    def _():
        @pl.loop(RETURNED, AROUND)
        def _(p):
            carry_copy(p).start()

        @pl.loop(0, AROUND)
        def _(p):
            add_suffix(p)
            round_copy(p).start()

    @block(1)
    def _():
        @pl.loop(0, AROUND)
        def _(p):
            add_suffix(p)
            suffix_copy(p, suffix).start()
            pass_up(AROUND + p)

        @pl.loop(2 * AROUND, pieces)
        def _(p):
            pass_up(p)

        @pl.loop(0, RETURNED)
        def _(p):
            whole_copy(p, whole).wait_recv()
            take_off(p, suffix)

        @pl.loop(RETURNED, AROUND)
        def _(p):
            carry_copy(p).wait_recv()

    @block(2)
    def _():
        lead = pieces - 2 * AROUND

        @pl.loop(AROUND, AROUND + lead)
        def _(p):
            pass_up(p)

        @pl.loop(0, AROUND)
        def _(p):
            whole_copy(p, whole).wait_recv()

            @pl.when(p < RETURNED)
            def _():
                whole_copy(p, whole).start()
            take_off(p, total)
            pass_up(AROUND + lead + p)

    @block(3)
    def _():
        @pl.loop(0, AROUND)
        def _(p):
            carry_copy(p).wait_recv()
            whole_copy(p, carried).start()

        @pl.loop(AROUND, pieces)
        def _(p):
            carry_copy(p).wait_recv()

    for side in (0, 1):
        @pl.when(has("lat", side))
        def _():
            for s in range(STEPS):
                lat_copy(s, 0, ni, 0, side).wait_send()

        @pl.when(has("lon", side))
        def _():
            for s in range(STEPS):
                lon_copy(s, side).wait_send()

        @pl.when(has("lev", side))
        def _():
            for s in range(STEPS):
                lev_copy(s, 0, ni, 0, side).wait_send()

    chain = pieces - AROUND

    @block(0)
    def _():
        carry_copy(0, pieces - RETURNED).wait_send()
        round_copy(0, AROUND).wait_send()

    @block(1)
    def _():
        carry_copy(0, chain).wait_send()
        suffix_copy(0, suffix, AROUND).wait_send()

    @block(2)
    def _():
        carry_copy(0, chain).wait_send()
        suffix_copy(0, total, AROUND).wait_send()
        whole_copy(0, whole, RETURNED).wait_send()

    @block(3)
    def _():
        whole_copy(0, carried, AROUND).wait_send()


def march(tracer, crowding, rows):
    nj, ni, nk, levels = tracer.shape
    chunks = ni // (2 * rows)
    f32 = jnp.float32
    dma = pltpu.SemaphoreType.DMA
    return pl.pallas_call(
        functools.partial(march_kernel, rows),
        out_shape=(jax.ShapeDtypeStruct(tracer.shape, f32), jax.ShapeDtypeStruct(tracer.shape[1:], f32)),
        in_specs=[pl.BlockSpec(memory_space=pl.ANY)] * 2,
        out_specs=(pl.BlockSpec(memory_space=pltpu.VMEM),) * 2,
        scratch_shapes=[
            pltpu.VMEM((STEPS, nj + 2, ni + 2, nk, levels), f32),
            pltpu.VMEM((nj, ni, nk, levels), f32),
            pltpu.VMEM((STEPS, 2, ni, nj, 1, levels), f32),
            pltpu.VMEM((STEPS, 2, ni, nj, 1, levels), f32),
            pltpu.VMEM((ni, nk, levels), f32),
            pltpu.VMEM((ni, nk, levels), f32),
            pltpu.VMEM((ni, nk, levels), f32),
            dma((2,)),
            dma((10,)),
            dma((STEPS, chunks, 2)),
            dma((STEPS, 2)),
            dma((STEPS, chunks, 2)),
            dma((2 * chunks,)),
            dma((AROUND,)),
            dma((AROUND,)),
        ],
        compiler_params=pltpu.CompilerParams(
            collective_id=0, has_side_effects=True, vmem_limit_bytes=48 * 2**20),
        name="march",
    )(tracer, crowding)


def sums_kernel(scale, block, end, carried, sums, copied, held, sem):
    nj, ni = end.shape[:2]
    blocks = ni // block

    def written(n, b):
        at_b = pl.ds(b * block, block)
        source, target = ((end, copied), (held, sums))[n]
        return pltpu.make_async_copy(source.at[:, at_b], target.at[:, at_b], sem.at[n, b])

    for b in range(blocks):
        written(0, b).start()
    for b in range(blocks):
        @pl.loop(b * block, (b + 1) * block)
        def _(i):
            run = carried[i]
            for j in range(nj):
                run = run + end[j, i]
                held[j, i] = run * scale
        written(1, b).start()
    for b in range(blocks):
        for n in (0, 1):
            written(n, b).wait()


def sums_along_j(end, carried, cells):
    ni = end.shape[1]
    block = min(8, ni)
    return pl.pallas_call(
        functools.partial(sums_kernel, 1.0 / cells, block),
        out_shape=(jax.ShapeDtypeStruct(end.shape, end.dtype),) * 2,
        in_specs=[pl.BlockSpec(memory_space=pltpu.VMEM)] * 2,
        out_specs=(pl.BlockSpec(memory_space=pl.ANY),) * 2,
        scratch_shapes=[pltpu.VMEM(end.shape, end.dtype), pltpu.SemaphoreType.DMA((2, ni // block))],
        compiler_params=pltpu.CompilerParams(vmem_limit_bytes=12 * 2**20),
        name="sums",
    )(end, carried)


def on_device(tracer, crowding):
    end, carried = march(tracer, crowding, min(ROWS, tracer.shape[1] // 2))
    return sums_along_j(end, carried, tracer.shape[0] * lax.axis_size("lat"))


def solution(mesh):
    spec = P(("unit", "lat"), "lon", "lev", None)
    return jax.shard_map(
        on_device, mesh=mesh, in_specs=(spec, spec), out_specs=(spec, spec), check_vma=False)
```

```python
import functools

import jax
import jax.numpy as jnp
from jax import lax
from jax.experimental import pallas as pl
from jax.experimental.pallas import tpu as pltpu
from jax.sharding import PartitionSpec as P

STEPS = 4
ROWS = 4
PIECE = 2
AROUND = 14
RETURNED = 8
LEAD = 9
MESH = pl.DeviceIdType.MESH
AXES = ("unit", "lat", "lon", "lev")


def march_kernel(rows, tracer, crowding, end, carried, t, c, faces, edges, total, suffix, whole,
                 load_sem, send_sem, lat_sem, lon_sem, lev_sem, carry_sem, suffix_sem, whole_sem,
                 go_sem):
    nj, ni, nk, levels = tracer.shape
    chunks = ni // (2 * rows)
    at = {axis: lax.axis_index(axis) for axis in AXES}
    size = {axis: lax.axis_size(axis) for axis in AXES}

    def has(axis, side):
        return at[axis] > 0 if side == 0 else at[axis] < size[axis] - 1

    def there(axis, side):
        return {axis: at[axis] - 1 if side == 0 else at[axis] + 1}

    def starts(m):
        return (m * rows, ni - (m + 1) * rows)

    def lat_copy(s, a, length, m, side, source=None):
        row = 0 if side == 0 else nj - 1
        if source is None:
            source = t.at[s, 1 + row, pl.ds(1 + a, length)]
        return pltpu.make_async_remote_copy(
            source, t.at[s, nj + 1 if side == 0 else 0, pl.ds(1 + a, length)],
            send_sem.at[side], lat_sem.at[s, m, 1 - side], device_id=there("lat", side), device_id_type=MESH)

    def lon_copy(s, side, source=None):
        if source is None:
            source = t.at[s, pl.ds(1, nj), 1 if side == 0 else ni]
        return pltpu.make_async_remote_copy(
            source, t.at[s, pl.ds(1, nj), ni + 1 if side == 0 else 0],
            send_sem.at[2 + side], lon_sem.at[s, 1 - side], device_id=there("lon", side), device_id_type=MESH)

    def lev_copy(s, a, length, m, side):
        return pltpu.make_async_remote_copy(
            faces.at[s, side, pl.ds(a, length)], edges.at[s, 1 - side, pl.ds(a, length)],
            send_sem.at[4 + side], lev_sem.at[s, m, 1 - side], device_id=there("lev", side), device_id_type=MESH)

    piece = min(PIECE, rows)
    half = rows // piece
    pieces = 2 * half * chunks
    assert 2 * AROUND <= pieces <= 2 * AROUND + LEAD
    last = size["lat"] - 1

    def span(p):
        m, n = p // (2 * half), p % (2 * half)
        start = jnp.where(n < half, m * rows, ni - (m + 1) * rows - rows)
        return pl.ds(start + n * piece, piece)

    def carry_copy(p, count=1):
        at_p = span(p) if count == 1 else pl.ds(0, count * piece)
        return pltpu.make_async_remote_copy(
            total.at[at_p], carried.at[at_p], send_sem.at[6], carry_sem.at[p],
            device_id=there("lat", 1), device_id_type=MESH)

    def suffix_copy(p, source, count=1):
        at_p = span(p) if count == 1 else pl.ds(0, count * piece)
        return pltpu.make_async_remote_copy(
            source.at[at_p], suffix.at[at_p], send_sem.at[7], suffix_sem.at[p],
            device_id=there("lat", 0), device_id_type=MESH)

    def round_copy(p, count=1):
        at_p = span(p) if count == 1 else pl.ds(0, count * piece)
        return pltpu.make_async_remote_copy(
            suffix.at[at_p], carried.at[at_p], send_sem.at[8], carry_sem.at[p],
            device_id={"lat": last}, device_id_type=MESH)

    def whole_copy(p, source, count=1):
        at_p = span(p) if count == 1 else pl.ds(0, count * piece)
        return pltpu.make_async_remote_copy(
            source.at[at_p], whole.at[at_p], send_sem.at[9], whole_sem.at[p],
            device_id=there("lat", 0), device_id_type=MESH)

    load_t = pltpu.make_async_copy(tracer, t.at[0, pl.ds(1, nj), pl.ds(1, ni)], load_sem.at[0])
    load_c = pltpu.make_async_copy(crowding, c, load_sem.at[1])

    barrier = pltpu.get_barrier_semaphore()

    def greet(where):
        pl.semaphore_signal(barrier, inc=1, device_id=where, device_id_type=MESH)

    def let_go(where):
        pl.semaphore_signal(go_sem, inc=1, device_id=where, device_id_type=MESH)

    def count(axis):
        return has(axis, 0).astype(jnp.int32) + has(axis, 1).astype(jnp.int32)

    odd = at["lev"] % 2 == 1
    even = at["lev"] % 2 == 0
    keeper = jnp.logical_and(even, at["lat"] == last)
    ends = jnp.logical_or(at["lat"] == 0, at["lat"] == last)
    between = jnp.logical_and(at["lat"] > 0, at["lat"] < last - 1)
    for axis in ("lat", "lon"):
        for side in (0, 1):
            pl.when(has(axis, side))(functools.partial(greet, there(axis, side)))
    pl.when(ends)(functools.partial(greet, {"lat": last - at["lat"]}))
    pl.when(jnp.logical_and(even, between))(functools.partial(greet, {"lat": last}))
    load_t.start()
    load_c.start()

    zero = jnp.zeros((nk, levels), jnp.float32)
    for side in (0, 1):
        @pl.when(jnp.logical_not(has("lat", side)))
        def _():
            @pl.loop(0, ni)
            def _(i):
                for s in range(STEPS):
                    t[s, 0 if side == 0 else nj + 1, 1 + i] = zero

            if side == 0:
                @pl.loop(0, ni)
                def _(i):
                    carried[i] = zero

        @pl.when(jnp.logical_not(has("lon", side)))
        def _():
            for s in range(STEPS):
                for j in range(nj):
                    t[s, 1 + j, 0 if side == 0 else ni + 1] = zero

        @pl.when(jnp.logical_not(has("lev", side)))
        def _():
            @pl.loop(0, ni)
            def _(i):
                for s in range(STEPS):
                    for j in range(nj):
                        edges[s, side, i, j] = jnp.zeros((1, levels), jnp.float32)

    near = count("lat") + count("lon") + ends.astype(jnp.int32)
    pl.semaphore_wait(
        barrier, near + jnp.where(keeper, last - 2 + size["lat"] * count("lev"), 0))
    for side in (0, 1):
        pl.when(jnp.logical_and(odd, has("lev", side)))(
            functools.partial(greet, {"lat": last, **there("lev", side)}))

    for m in range(chunks):
        for side in (0, 1):
            @pl.when(has("lat", side))
            def _():
                for a in starts(m):
                    lat_copy(0, a, rows, m, side,
                             tracer.at[0 if side == 0 else nj - 1, pl.ds(a, rows)]).start()
    for side in (0, 1):
        @pl.when(has("lon", side))
        def _():
            lon_copy(0, side, tracer.at[:, 0 if side == 0 else ni - 1]).start()

    @pl.when(keeper)
    def _():
        for n in range(last):
            let_go({"lat": n})

    @pl.when(jnp.logical_and(even, at["lat"] < last))
    def _():
        pl.semaphore_wait(go_sem, 1)

    for side in (0, 1):
        pl.when(jnp.logical_and(even, has("lev", side)))(functools.partial(let_go, there("lev", side)))

    def send_lev(s, m):
        for side in (0, 1):
            @pl.when(has("lev", side))
            def _():
                for a in starts(m):
                    lev_copy(s, a, rows, m, side).start()

    load_t.wait()

    @pl.loop(0, chunks)
    def _(m):
        @pl.loop(0, rows)
        def _(r):
            for a in starts(m):
                for j in range(nj):
                    faces[0, 0, a + r, j] = t[0, 1 + j, 1 + a + r, 0:1]
                    faces[0, 1, a + r, j] = t[0, 1 + j, 1 + a + r, nk - 1:nk]

    @pl.when(odd)
    def _():
        pl.semaphore_wait(go_sem, count("lev"))

    @pl.loop(0, chunks)
    def _(m):
        send_lev(0, m)

    load_c.wait()

    below = lax.broadcasted_iota(jnp.int32, (nk, levels), 0) == 0
    above = lax.broadcasted_iota(jnp.int32, (nk, levels), 0) == nk - 1

    def stepped(s, i):
        for j in range(nj):
            middle = t[s, 1 + j, 1 + i]
            lower = jnp.where(below, edges[s, 0, i, j], pltpu.roll(middle, 1, 0))
            upper = jnp.where(above, edges[s, 1, i, j], pltpu.roll(middle, nk - 1, 0))
            spread = (t[s, j, 1 + i] + t[s, 2 + j, 1 + i] + t[s, 1 + j, i] + t[s, 1 + j, 2 + i]
                      + lower + upper - 6.0 * middle)
            yield j, middle + 0.1 * spread + 0.2 * middle * (1.0 - middle * c[j, i])

    def arrived(s, m):
        for side in (0, 1):
            @pl.when(has("lat", side))
            def _():
                lat_copy(s, 0, 2 * rows, m, 1 - side).wait_recv()

            @pl.when(has("lev", side))
            def _():
                lev_copy(s, 0, 2 * rows, m, 1 - side).wait_recv()

            @pl.when(jnp.logical_and(has("lon", side), m == 0))
            def _():
                lon_copy(s, 1 - side).wait_recv()

    @pl.loop(0, STEPS - 1)
    def _(s):
        @pl.loop(0, chunks)
        def _(m):
            arrived(s, m)

            @pl.loop(0, rows)
            def _(r):
                for a in starts(m):
                    for j, value in stepped(s, a + r):
                        t[s + 1, 1 + j, 1 + a + r] = value
                        faces[s + 1, 0, a + r, j] = value[0:1]
                        faces[s + 1, 1, a + r, j] = value[nk - 1:nk]

            for side in (0, 1):
                @pl.when(has("lat", side))
                def _():
                    for a in starts(m):
                        lat_copy(s + 1, a, rows, m, side).start()
            send_lev(s + 1, m)
            for side in (0, 1):
                @pl.when(jnp.logical_and(has("lon", side), m == 0))
                def _():
                    lon_copy(s + 1, side).start()

    def block(n):
        return pl.when(at["lat"] == n)

    @pl.loop(0, chunks)
    def _(m):
        arrived(STEPS - 1, m)

        @pl.loop(0, rows)
        def _(r):
            for a in starts(m):
                summed = None
                for j, value in stepped(STEPS - 1, a + r):
                    end[j, a + r] = value
                    summed = value if j == 0 else summed + value
                total[a + r] = summed

        for n in range(2 * half):
            p = 2 * half * m + n

            @pl.when(jnp.logical_and(at["lat"] == 0, p >= AROUND))
            def _():
                carry_copy(p).start()

            @pl.when(jnp.logical_and(at["lat"] == last - 1, p < AROUND))
            def _():
                suffix_copy(p, total).start()

    def add_suffix(p):
        suffix_copy(p, suffix).wait_recv()

        for r in range(piece):
            i = span(p).start + r
            suffix[i] = suffix[i] + total[i]

    def pass_up(p):
        carry_copy(p).wait_recv()

        for r in range(piece):
            i = span(p).start + r
            total[i] = total[i] + carried[i]
        carry_copy(p).start()

    def take_off(p, own):
        for r in range(piece):
            i = span(p).start + r
            carried[i] = whole[i] - own[i]

    @block(0)
    def _():
        @pl.loop(RETURNED, AROUND)
        def _(p):
            carry_copy(p).start()

        @pl.loop(0, AROUND)
        def _(p):
            add_suffix(p)
            round_copy(p).start()

    @block(1)
    def _():
        @pl.loop(0, AROUND)
        def _(p):
            add_suffix(p)
            suffix_copy(p, suffix).start()
            pass_up(AROUND + p)

        @pl.loop(2 * AROUND, pieces)
        def _(p):
            pass_up(p)

        @pl.loop(0, RETURNED)
        def _(p):
            whole_copy(p, whole).wait_recv()
            take_off(p, suffix)

        @pl.loop(RETURNED, AROUND)
        def _(p):
            carry_copy(p).wait_recv()

    @block(2)
    def _():
        paired = pieces - AROUND - LEAD

        def take_whole(p):
            whole_copy(p, whole).wait_recv()

            @pl.when(p < RETURNED)
            def _():
                whole_copy(p, whole).start()
            take_off(p, total)

        @pl.loop(AROUND, AROUND + LEAD)
        def _(p):
            pass_up(p)

        @pl.loop(0, paired)
        def _(p):
            pass_up(AROUND + LEAD + p)
            take_whole(p)

        @pl.loop(paired, AROUND)
        def _(p):
            take_whole(p)

    @block(3)
    def _():
        @pl.loop(0, AROUND)
        def _(p):
            carry_copy(p).wait_recv()
            whole_copy(p, carried).start()

        @pl.loop(AROUND, pieces)
        def _(p):
            carry_copy(p).wait_recv()

    for side in (0, 1):
        @pl.when(has("lat", side))
        def _():
            for s in range(STEPS):
                lat_copy(s, 0, ni, 0, side).wait_send()

        @pl.when(has("lon", side))
        def _():
            for s in range(STEPS):
                lon_copy(s, side).wait_send()

        @pl.when(has("lev", side))
        def _():
            for s in range(STEPS):
                lev_copy(s, 0, ni, 0, side).wait_send()

    chain = pieces - AROUND

    @block(0)
    def _():
        carry_copy(0, pieces - RETURNED).wait_send()
        round_copy(0, AROUND).wait_send()

    @block(1)
    def _():
        carry_copy(0, chain).wait_send()
        suffix_copy(0, suffix, AROUND).wait_send()

    @block(2)
    def _():
        carry_copy(0, chain).wait_send()
        suffix_copy(0, total, AROUND).wait_send()
        whole_copy(0, whole, RETURNED).wait_send()

    @block(3)
    def _():
        whole_copy(0, carried, AROUND).wait_send()


def march(tracer, crowding, rows):
    nj, ni, nk, levels = tracer.shape
    chunks = ni // (2 * rows)
    f32 = jnp.float32
    dma = pltpu.SemaphoreType.DMA
    return pl.pallas_call(
        functools.partial(march_kernel, rows),
        out_shape=(jax.ShapeDtypeStruct(tracer.shape, f32), jax.ShapeDtypeStruct(tracer.shape[1:], f32)),
        in_specs=[pl.BlockSpec(memory_space=pl.ANY)] * 2,
        out_specs=(pl.BlockSpec(memory_space=pltpu.VMEM),) * 2,
        scratch_shapes=[
            pltpu.VMEM((STEPS, nj + 2, ni + 2, nk, levels), f32),
            pltpu.VMEM((nj, ni, nk, levels), f32),
            pltpu.VMEM((STEPS, 2, ni, nj, 1, levels), f32),
            pltpu.VMEM((STEPS, 2, ni, nj, 1, levels), f32),
            pltpu.VMEM((ni, nk, levels), f32),
            pltpu.VMEM((ni, nk, levels), f32),
            pltpu.VMEM((ni, nk, levels), f32),
            dma((2,)),
            dma((10,)),
            dma((STEPS, chunks, 2)),
            dma((STEPS, 2)),
            dma((STEPS, chunks, 2)),
            dma((ni // min(PIECE, rows),)),
            dma((AROUND,)),
            dma((AROUND,)),
            pltpu.SemaphoreType.REGULAR,
        ],
        compiler_params=pltpu.CompilerParams(
            collective_id=0, has_side_effects=True, vmem_limit_bytes=48 * 2**20),
        name="march",
    )(tracer, crowding)


def sums_kernel(scale, block, end, carried, sums, copied, held, sem):
    nj, ni = end.shape[:2]
    blocks = ni // block

    def written(n, b):
        at_b = pl.ds(b * block, block)
        source, target = ((end, copied), (held, sums))[n]
        return pltpu.make_async_copy(source.at[:, at_b], target.at[:, at_b], sem.at[n, b])

    for b in range(blocks):
        written(0, b).start()
    for b in range(blocks):
        @pl.loop(b * block, (b + 1) * block)
        def _(i):
            run = carried[i]
            for j in range(nj):
                run = run + end[j, i]
                held[j, i] = run * scale
        written(1, b).start()
    for b in range(blocks):
        for n in (0, 1):
            written(n, b).wait()


def sums_along_j(end, carried, cells):
    ni = end.shape[1]
    block = min(8, ni)
    return pl.pallas_call(
        functools.partial(sums_kernel, 1.0 / cells, block),
        out_shape=(jax.ShapeDtypeStruct(end.shape, end.dtype),) * 2,
        in_specs=[pl.BlockSpec(memory_space=pltpu.VMEM)] * 2,
        out_specs=(pl.BlockSpec(memory_space=pl.ANY),) * 2,
        scratch_shapes=[pltpu.VMEM(end.shape, end.dtype), pltpu.SemaphoreType.DMA((2, ni // block))],
        compiler_params=pltpu.CompilerParams(vmem_limit_bytes=12 * 2**20),
        name="sums",
    )(end, carried)


def on_device(tracer, crowding):
    end, carried = march(tracer, crowding, min(ROWS, tracer.shape[1] // 2))
    return sums_along_j(end, carried, tracer.shape[0] * lax.axis_size("lat"))


def solution(mesh):
    spec = P(("unit", "lat"), "lon", "lev", None)
    return jax.shard_map(
        on_device, mesh=mesh, in_specs=(spec, spec), out_specs=(spec, spec), check_vma=False)
```

```python
import functools

import jax
import jax.numpy as jnp
from jax import lax
from jax.experimental import pallas as pl
from jax.experimental.pallas import tpu as pltpu
from jax.sharding import PartitionSpec as P

STEPS = 4
ROWS = 4
PIECE = 2
SPLIT = 7
ROUND = 14
CHAIN = 18
RETURNED = 10
LEAD = 5
MESH = pl.DeviceIdType.MESH
AXES = ("unit", "lat", "lon", "lev")


def march_kernel(rows, tracer, crowding, end, carried, t, c, faces, edges, total, suffix, whole,
                 load_sem, send_sem, lat_sem, lon_sem, lev_sem, carry_sem, suffix_sem, whole_sem,
                 go_sem):
    nj, ni, nk, levels = tracer.shape
    chunks = ni // (2 * rows)
    at = {axis: lax.axis_index(axis) for axis in AXES}
    size = {axis: lax.axis_size(axis) for axis in AXES}

    def has(axis, side):
        return at[axis] > 0 if side == 0 else at[axis] < size[axis] - 1

    def there(axis, side):
        return {axis: at[axis] - 1 if side == 0 else at[axis] + 1}

    def starts(m):
        return (m * rows, ni - (m + 1) * rows)

    def lat_copy(s, a, length, m, side, source=None):
        row = 0 if side == 0 else nj - 1
        if source is None:
            source = t.at[s, 1 + row, pl.ds(1 + a, length)]
        return pltpu.make_async_remote_copy(
            source, t.at[s, nj + 1 if side == 0 else 0, pl.ds(1 + a, length)],
            send_sem.at[side], lat_sem.at[s, m, 1 - side], device_id=there("lat", side), device_id_type=MESH)

    def lon_copy(s, side, source=None):
        if source is None:
            source = t.at[s, pl.ds(1, nj), 1 if side == 0 else ni]
        return pltpu.make_async_remote_copy(
            source, t.at[s, pl.ds(1, nj), ni + 1 if side == 0 else 0],
            send_sem.at[2 + side], lon_sem.at[s, 1 - side], device_id=there("lon", side), device_id_type=MESH)

    def lev_copy(s, a, length, m, side):
        return pltpu.make_async_remote_copy(
            faces.at[s, side, pl.ds(a, length)], edges.at[s, 1 - side, pl.ds(a, length)],
            send_sem.at[4 + side], lev_sem.at[s, m, 1 - side], device_id=there("lev", side), device_id_type=MESH)

    piece = min(PIECE, rows)
    half = rows // piece
    pieces = 2 * half * chunks
    assert CHAIN - SPLIT <= pieces - CHAIN <= ROUND + LEAD
    last = size["lat"] - 1

    def span(p):
        m, n = p // (2 * half), p % (2 * half)
        start = jnp.where(n < half, m * rows, ni - (m + 1) * rows - rows)
        return pl.ds(start + n * piece, piece)

    def carry_copy(p, count=1):
        at_p = span(p) if count == 1 else pl.ds(0, count * piece)
        return pltpu.make_async_remote_copy(
            total.at[at_p], carried.at[at_p], send_sem.at[6], carry_sem.at[p],
            device_id=there("lat", 1), device_id_type=MESH)

    def suffix_copy(p, source, count=1):
        at_p = span(p) if count == 1 else pl.ds(0, count * piece)
        return pltpu.make_async_remote_copy(
            source.at[at_p], suffix.at[at_p], send_sem.at[7], suffix_sem.at[p],
            device_id=there("lat", 0), device_id_type=MESH)

    def round_copy(p, count=1):
        at_p = span(p) if count == 1 else pl.ds(0, count * piece)
        return pltpu.make_async_remote_copy(
            suffix.at[at_p], whole.at[at_p], send_sem.at[8], whole_sem.at[p],
            device_id={"lat": last}, device_id_type=MESH)

    def whole_copy(p, count=1):
        at_p = span(p) if count == 1 else pl.ds(0, count * piece)
        return pltpu.make_async_remote_copy(
            whole.at[at_p], whole.at[at_p], send_sem.at[9], whole_sem.at[p],
            device_id=there("lat", 0), device_id_type=MESH)

    load_t = pltpu.make_async_copy(tracer, t.at[0, pl.ds(1, nj), pl.ds(1, ni)], load_sem.at[0])
    load_c = pltpu.make_async_copy(crowding, c, load_sem.at[1])

    barrier = pltpu.get_barrier_semaphore()

    def greet(where):
        pl.semaphore_signal(barrier, inc=1, device_id=where, device_id_type=MESH)

    def let_go(where):
        pl.semaphore_signal(go_sem, inc=1, device_id=where, device_id_type=MESH)

    def count(axis):
        return has(axis, 0).astype(jnp.int32) + has(axis, 1).astype(jnp.int32)

    odd = at["lev"] % 2 == 1
    even = at["lev"] % 2 == 0
    keeper = jnp.logical_and(even, at["lat"] == last)
    ends = jnp.logical_or(at["lat"] == 0, at["lat"] == last)
    between = jnp.logical_and(at["lat"] > 0, at["lat"] < last - 1)
    for axis in ("lat", "lon"):
        for side in (0, 1):
            pl.when(has(axis, side))(functools.partial(greet, there(axis, side)))
    pl.when(ends)(functools.partial(greet, {"lat": last - at["lat"]}))
    pl.when(jnp.logical_and(even, between))(functools.partial(greet, {"lat": last}))
    load_t.start()
    load_c.start()

    zero = jnp.zeros((nk, levels), jnp.float32)
    for side in (0, 1):
        @pl.when(jnp.logical_not(has("lat", side)))
        def _():
            @pl.loop(0, ni)
            def _(i):
                for s in range(STEPS):
                    t[s, 0 if side == 0 else nj + 1, 1 + i] = zero

            if side == 0:
                @pl.loop(0, ni)
                def _(i):
                    carried[i] = zero

        @pl.when(jnp.logical_not(has("lon", side)))
        def _():
            for s in range(STEPS):
                for j in range(nj):
                    t[s, 1 + j, 0 if side == 0 else ni + 1] = zero

        @pl.when(jnp.logical_not(has("lev", side)))
        def _():
            @pl.loop(0, ni)
            def _(i):
                for s in range(STEPS):
                    for j in range(nj):
                        edges[s, side, i, j] = jnp.zeros((1, levels), jnp.float32)

    near = count("lat") + count("lon") + ends.astype(jnp.int32)
    pl.semaphore_wait(
        barrier, near + jnp.where(keeper, last - 2 + size["lat"] * count("lev"), 0))
    for side in (0, 1):
        pl.when(jnp.logical_and(odd, has("lev", side)))(
            functools.partial(greet, {"lat": last, **there("lev", side)}))

    for m in range(chunks):
        for side in (0, 1):
            @pl.when(has("lat", side))
            def _():
                for a in starts(m):
                    lat_copy(0, a, rows, m, side,
                             tracer.at[0 if side == 0 else nj - 1, pl.ds(a, rows)]).start()
    for side in (0, 1):
        @pl.when(has("lon", side))
        def _():
            lon_copy(0, side, tracer.at[:, 0 if side == 0 else ni - 1]).start()

    @pl.when(keeper)
    def _():
        for n in range(last):
            let_go({"lat": n})

    @pl.when(jnp.logical_and(even, at["lat"] < last))
    def _():
        pl.semaphore_wait(go_sem, 1)

    for side in (0, 1):
        pl.when(jnp.logical_and(even, has("lev", side)))(functools.partial(let_go, there("lev", side)))

    def send_lev(s, m):
        for side in (0, 1):
            @pl.when(has("lev", side))
            def _():
                for a in starts(m):
                    lev_copy(s, a, rows, m, side).start()

    load_t.wait()

    @pl.loop(0, chunks)
    def _(m):
        @pl.loop(0, rows)
        def _(r):
            for a in starts(m):
                for j in range(nj):
                    faces[0, 0, a + r, j] = t[0, 1 + j, 1 + a + r, 0:1]
                    faces[0, 1, a + r, j] = t[0, 1 + j, 1 + a + r, nk - 1:nk]

    @pl.when(odd)
    def _():
        pl.semaphore_wait(go_sem, count("lev"))

    @pl.loop(0, chunks)
    def _(m):
        send_lev(0, m)

    load_c.wait()

    below = lax.broadcasted_iota(jnp.int32, (nk, levels), 0) == 0
    above = lax.broadcasted_iota(jnp.int32, (nk, levels), 0) == nk - 1

    def stepped(s, i):
        for j in range(nj):
            middle = t[s, 1 + j, 1 + i]
            lower = jnp.where(below, edges[s, 0, i, j], pltpu.roll(middle, 1, 0))
            upper = jnp.where(above, edges[s, 1, i, j], pltpu.roll(middle, nk - 1, 0))
            spread = (t[s, j, 1 + i] + t[s, 2 + j, 1 + i] + t[s, 1 + j, i] + t[s, 1 + j, 2 + i]
                      + lower + upper - 6.0 * middle)
            yield j, middle + 0.1 * spread + 0.2 * middle * (1.0 - middle * c[j, i])

    def arrived(s, m):
        for side in (0, 1):
            @pl.when(has("lat", side))
            def _():
                lat_copy(s, 0, 2 * rows, m, 1 - side).wait_recv()

            @pl.when(has("lev", side))
            def _():
                lev_copy(s, 0, 2 * rows, m, 1 - side).wait_recv()

            @pl.when(jnp.logical_and(has("lon", side), m == 0))
            def _():
                lon_copy(s, 1 - side).wait_recv()

    @pl.loop(0, STEPS - 1)
    def _(s):
        @pl.loop(0, chunks)
        def _(m):
            arrived(s, m)

            @pl.loop(0, rows)
            def _(r):
                for a in starts(m):
                    for j, value in stepped(s, a + r):
                        t[s + 1, 1 + j, 1 + a + r] = value
                        faces[s + 1, 0, a + r, j] = value[0:1]
                        faces[s + 1, 1, a + r, j] = value[nk - 1:nk]

            for side in (0, 1):
                @pl.when(has("lat", side))
                def _():
                    for a in starts(m):
                        lat_copy(s + 1, a, rows, m, side).start()
            send_lev(s + 1, m)
            for side in (0, 1):
                @pl.when(jnp.logical_and(has("lon", side), m == 0))
                def _():
                    lon_copy(s + 1, side).start()

    def block(n):
        return pl.when(at["lat"] == n)

    @pl.loop(0, chunks)
    def _(m):
        arrived(STEPS - 1, m)

        @pl.loop(0, rows)
        def _(r):
            for a in starts(m):
                summed = None
                for j, value in stepped(STEPS - 1, a + r):
                    end[j, a + r] = value
                    summed = value if j == 0 else summed + value
                total[a + r] = summed

        for n in range(2 * half):
            p = 2 * half * m + n

            up = jnp.logical_or(jnp.logical_and(at["lat"] == 0, p >= CHAIN),
                                jnp.logical_and(at["lat"] == 2, p < SPLIT))
            down = jnp.logical_or(jnp.logical_and(at["lat"] == 1, p < SPLIT),
                                  jnp.logical_and(at["lat"] == 2, jnp.logical_and(p >= SPLIT, p < CHAIN)))

            @pl.when(up)
            def _():
                carry_copy(p).start()

            @pl.when(down)
            def _():
                suffix_copy(p, total).start()

    def combine(p, target, value):
        for r in range(piece):
            i = span(p).start + r
            target[i] = value(i)

    def add_suffix(p):
        suffix_copy(p, suffix).wait_recv()
        combine(p, suffix, lambda i: suffix[i] + total[i])

    def pass_up(p):
        carry_copy(p).wait_recv()
        combine(p, total, lambda i: total[i] + carried[i])
        carry_copy(p).start()

    @block(0)
    def _():
        @pl.loop(ROUND, CHAIN)
        def _(p):
            carry_copy(p).start()

        @pl.loop(RETURNED, ROUND)
        def _(p):
            carry_copy(p).start()

        @pl.loop(0, CHAIN)
        def _(p):
            add_suffix(p)
            round_copy(p).start()

    @block(1)
    def _():
        @pl.loop(SPLIT, CHAIN)
        def _(p):
            add_suffix(p)
            suffix_copy(p, suffix).start()
            pass_up(CHAIN - SPLIT + p)

        @pl.loop(2 * CHAIN - SPLIT, pieces)
        def _(p):
            pass_up(p)

        @pl.loop(ROUND, CHAIN)
        def _(p):
            pass_up(p)

        @pl.loop(0, SPLIT)
        def _(p):
            whole_copy(p).wait_recv()
            combine(p, carried, lambda i: whole[i] - total[i])

        @pl.loop(SPLIT, RETURNED)
        def _(p):
            whole_copy(p).wait_recv()
            combine(p, carried, lambda i: whole[i] - suffix[i])

        @pl.loop(RETURNED, ROUND)
        def _(p):
            carry_copy(p).wait_recv()

    @block(2)
    def _():
        paired = pieces - CHAIN - LEAD

        def take_whole(p):
            whole_copy(p).wait_recv()

            @pl.when(p < RETURNED)
            def _():
                whole_copy(p).start()

            @pl.when(p < SPLIT)
            def _():
                combine(p, carried, lambda i: whole[i])

            @pl.when(p >= SPLIT)
            def _():
                combine(p, carried, lambda i: whole[i] - total[i])

        @pl.loop(CHAIN, CHAIN + LEAD)
        def _(p):
            pass_up(p)

        @pl.loop(0, paired)
        def _(p):
            pass_up(CHAIN + LEAD + p)
            take_whole(p)

        @pl.loop(paired, ROUND)
        def _(p):
            take_whole(p)

        @pl.loop(ROUND, CHAIN)
        def _(p):
            carry_copy(p).wait_recv()

    @block(3)
    def _():
        @pl.loop(0, SPLIT)
        def _(p):
            whole_copy(p).wait_recv()
            whole_copy(p).start()
            carry_copy(p).wait_recv()
            combine(p, carried, lambda i: carried[i] + whole[i])

        @pl.loop(SPLIT, CHAIN)
        def _(p):
            whole_copy(p).wait_recv()

            @pl.when(p < ROUND)
            def _():
                whole_copy(p).start()
            combine(p, carried, lambda i: whole[i])

        @pl.loop(CHAIN, pieces)
        def _(p):
            carry_copy(p).wait_recv()

    for side in (0, 1):
        @pl.when(has("lat", side))
        def _():
            for s in range(STEPS):
                lat_copy(s, 0, ni, 0, side).wait_send()

        @pl.when(has("lon", side))
        def _():
            for s in range(STEPS):
                lon_copy(s, side).wait_send()

        @pl.when(has("lev", side))
        def _():
            for s in range(STEPS):
                lev_copy(s, 0, ni, 0, side).wait_send()

    chain = pieces - CHAIN

    @block(0)
    def _():
        carry_copy(0, chain + CHAIN - RETURNED).wait_send()
        round_copy(0, CHAIN).wait_send()

    @block(1)
    def _():
        carry_copy(0, chain + CHAIN - ROUND).wait_send()
        suffix_copy(0, suffix, CHAIN).wait_send()

    @block(2)
    def _():
        carry_copy(0, chain + SPLIT).wait_send()
        suffix_copy(0, total, CHAIN - SPLIT).wait_send()
        whole_copy(0, RETURNED).wait_send()

    @block(3)
    def _():
        whole_copy(0, ROUND).wait_send()


def march(tracer, crowding, rows):
    nj, ni, nk, levels = tracer.shape
    chunks = ni // (2 * rows)
    f32 = jnp.float32
    dma = pltpu.SemaphoreType.DMA
    return pl.pallas_call(
        functools.partial(march_kernel, rows),
        out_shape=(jax.ShapeDtypeStruct(tracer.shape, f32), jax.ShapeDtypeStruct(tracer.shape[1:], f32)),
        in_specs=[pl.BlockSpec(memory_space=pl.ANY)] * 2,
        out_specs=(pl.BlockSpec(memory_space=pltpu.VMEM),) * 2,
        scratch_shapes=[
            pltpu.VMEM((STEPS, nj + 2, ni + 2, nk, levels), f32),
            pltpu.VMEM((nj, ni, nk, levels), f32),
            pltpu.VMEM((STEPS, 2, ni, nj, 1, levels), f32),
            pltpu.VMEM((STEPS, 2, ni, nj, 1, levels), f32),
            pltpu.VMEM((ni, nk, levels), f32),
            pltpu.VMEM((ni, nk, levels), f32),
            pltpu.VMEM((ni, nk, levels), f32),
            dma((2,)),
            dma((10,)),
            dma((STEPS, chunks, 2)),
            dma((STEPS, 2)),
            dma((STEPS, chunks, 2)),
            dma((ni // min(PIECE, rows),)),
            dma((CHAIN,)),
            dma((CHAIN,)),
            pltpu.SemaphoreType.REGULAR,
        ],
        compiler_params=pltpu.CompilerParams(
            collective_id=0, has_side_effects=True, vmem_limit_bytes=48 * 2**20),
        name="march",
    )(tracer, crowding)


def sums_kernel(scale, block, end, carried, sums, copied, held, sem):
    nj, ni = end.shape[:2]
    blocks = ni // block

    def written(n, b):
        at_b = pl.ds(b * block, block)
        source, target = ((end, copied), (held, sums))[n]
        return pltpu.make_async_copy(source.at[:, at_b], target.at[:, at_b], sem.at[n, b])

    for b in range(blocks):
        written(0, b).start()
    for b in range(blocks):
        @pl.loop(b * block, (b + 1) * block)
        def _(i):
            run = carried[i]
            for j in range(nj):
                run = run + end[j, i]
                held[j, i] = run * scale
        written(1, b).start()
    for b in range(blocks):
        for n in (0, 1):
            written(n, b).wait()


def sums_along_j(end, carried, cells):
    ni = end.shape[1]
    block = min(8, ni)
    return pl.pallas_call(
        functools.partial(sums_kernel, 1.0 / cells, block),
        out_shape=(jax.ShapeDtypeStruct(end.shape, end.dtype),) * 2,
        in_specs=[pl.BlockSpec(memory_space=pltpu.VMEM)] * 2,
        out_specs=(pl.BlockSpec(memory_space=pl.ANY),) * 2,
        scratch_shapes=[pltpu.VMEM(end.shape, end.dtype), pltpu.SemaphoreType.DMA((2, ni // block))],
        compiler_params=pltpu.CompilerParams(vmem_limit_bytes=12 * 2**20),
        name="sums",
    )(end, carried)


def on_device(tracer, crowding):
    end, carried = march(tracer, crowding, min(ROWS, tracer.shape[1] // 2))
    return sums_along_j(end, carried, tracer.shape[0] * lax.axis_size("lat"))


def solution(mesh):
    spec = P(("unit", "lat"), "lon", "lev", None)
    return jax.shard_map(
        on_device, mesh=mesh, in_specs=(spec, spec), out_specs=(spec, spec), check_vma=False)
```

```python
import functools

import jax
import jax.numpy as jnp
from jax import lax
from jax.experimental import pallas as pl
from jax.experimental.pallas import tpu as pltpu
from jax.sharding import PartitionSpec as P

STEPS = 4
ROWS = 8
PIECE = 2
SPLIT = 8
ROUND = 14
CHAIN = 19
RETURNED = 9
LEAD = 5
MESH = pl.DeviceIdType.MESH
AXES = ("unit", "lat", "lon", "lev")


def march_kernel(rows, tracer, crowding, end, carried, t, c, faces, edges, total, suffix, whole,
                 load_sem, send_sem, lat_sem, lon_sem, lev_sem, carry_sem, suffix_sem, whole_sem,
                 go_sem):
    nj, ni, nk, levels = tracer.shape
    chunks = ni // (2 * rows)
    at = {axis: lax.axis_index(axis) for axis in AXES}
    size = {axis: lax.axis_size(axis) for axis in AXES}

    def has(axis, side):
        return at[axis] > 0 if side == 0 else at[axis] < size[axis] - 1

    def there(axis, side):
        return {axis: at[axis] - 1 if side == 0 else at[axis] + 1}

    def starts(m):
        return (m * rows, ni - (m + 1) * rows)

    def lat_copy(s, a, length, m, side, source=None):
        row = 0 if side == 0 else nj - 1
        if source is None:
            source = t.at[s, 1 + row, pl.ds(1 + a, length)]
        return pltpu.make_async_remote_copy(
            source, t.at[s, nj + 1 if side == 0 else 0, pl.ds(1 + a, length)],
            send_sem.at[side], lat_sem.at[s, m, 1 - side], device_id=there("lat", side), device_id_type=MESH)

    def lon_copy(s, side, source=None):
        if source is None:
            source = t.at[s, pl.ds(1, nj), 1 if side == 0 else ni]
        return pltpu.make_async_remote_copy(
            source, t.at[s, pl.ds(1, nj), ni + 1 if side == 0 else 0],
            send_sem.at[2 + side], lon_sem.at[s, 1 - side], device_id=there("lon", side), device_id_type=MESH)

    def lev_copy(s, a, length, m, side):
        return pltpu.make_async_remote_copy(
            faces.at[s, side, pl.ds(a, length)], edges.at[s, 1 - side, pl.ds(a, length)],
            send_sem.at[4 + side], lev_sem.at[s, m, 1 - side], device_id=there("lev", side), device_id_type=MESH)

    piece = min(PIECE, rows)
    half = rows // piece
    pieces = 2 * half * chunks
    assert CHAIN - SPLIT <= pieces - CHAIN <= ROUND + LEAD
    last = size["lat"] - 1

    def span(p):
        m, n = p // (2 * half), p % (2 * half)
        start = jnp.where(n < half, m * rows, ni - (m + 1) * rows - rows)
        return pl.ds(start + n * piece, piece)

    def carry_copy(p, count=1):
        at_p = span(p) if count == 1 else pl.ds(0, count * piece)
        return pltpu.make_async_remote_copy(
            total.at[at_p], carried.at[at_p], send_sem.at[6], carry_sem.at[p],
            device_id=there("lat", 1), device_id_type=MESH)

    def suffix_copy(p, source, count=1):
        at_p = span(p) if count == 1 else pl.ds(0, count * piece)
        return pltpu.make_async_remote_copy(
            source.at[at_p], suffix.at[at_p], send_sem.at[7], suffix_sem.at[p],
            device_id=there("lat", 0), device_id_type=MESH)

    def round_copy(p, count=1):
        at_p = span(p) if count == 1 else pl.ds(0, count * piece)
        return pltpu.make_async_remote_copy(
            suffix.at[at_p], whole.at[at_p], send_sem.at[8], whole_sem.at[p],
            device_id={"lat": last}, device_id_type=MESH)

    def whole_copy(p, count=1):
        at_p = span(p) if count == 1 else pl.ds(0, count * piece)
        return pltpu.make_async_remote_copy(
            whole.at[at_p], whole.at[at_p], send_sem.at[9], whole_sem.at[p],
            device_id=there("lat", 0), device_id_type=MESH)

    load_t = pltpu.make_async_copy(tracer, t.at[0, pl.ds(1, nj), pl.ds(1, ni)], load_sem.at[0])
    load_c = pltpu.make_async_copy(crowding, c, load_sem.at[1])

    barrier = pltpu.get_barrier_semaphore()

    def greet(where):
        pl.semaphore_signal(barrier, inc=1, device_id=where, device_id_type=MESH)

    def let_go(where):
        pl.semaphore_signal(go_sem, inc=1, device_id=where, device_id_type=MESH)

    def count(axis):
        return has(axis, 0).astype(jnp.int32) + has(axis, 1).astype(jnp.int32)

    odd = at["lev"] % 2 == 1
    even = at["lev"] % 2 == 0
    keeper = jnp.logical_and(even, at["lat"] == last)
    ends = jnp.logical_or(at["lat"] == 0, at["lat"] == last)
    between = jnp.logical_and(at["lat"] > 0, at["lat"] < last - 1)
    for axis in ("lat", "lon"):
        for side in (0, 1):
            pl.when(has(axis, side))(functools.partial(greet, there(axis, side)))
    pl.when(ends)(functools.partial(greet, {"lat": last - at["lat"]}))
    pl.when(jnp.logical_and(even, between))(functools.partial(greet, {"lat": last}))
    load_t.start()
    load_c.start()

    near = count("lat") + count("lon") + ends.astype(jnp.int32)
    pl.semaphore_wait(
        barrier, near + jnp.where(keeper, last - 2 + size["lat"] * count("lev"), 0))
    for side in (0, 1):
        pl.when(jnp.logical_and(odd, has("lev", side)))(
            functools.partial(greet, {"lat": last, **there("lev", side)}))

    for m in range(chunks):
        for side in (0, 1):
            @pl.when(has("lat", side))
            def _():
                for a in starts(m):
                    lat_copy(0, a, rows, m, side,
                             tracer.at[0 if side == 0 else nj - 1, pl.ds(a, rows)]).start()
    for side in (0, 1):
        @pl.when(has("lon", side))
        def _():
            lon_copy(0, side, tracer.at[:, 0 if side == 0 else ni - 1]).start()

    @pl.when(keeper)
    def _():
        for n in range(last):
            let_go({"lat": n})

    zero = jnp.zeros((nk, levels), jnp.float32)
    for side in (0, 1):
        @pl.when(jnp.logical_not(has("lat", side)))
        def _():
            @pl.loop(0, ni)
            def _(i):
                for s in range(STEPS):
                    t[s, 0 if side == 0 else nj + 1, 1 + i] = zero

            if side == 0:
                @pl.loop(0, ni)
                def _(i):
                    carried[i] = zero

        @pl.when(jnp.logical_not(has("lon", side)))
        def _():
            for s in range(STEPS):
                for j in range(nj):
                    t[s, 1 + j, 0 if side == 0 else ni + 1] = zero

        @pl.when(jnp.logical_not(has("lev", side)))
        def _():
            @pl.loop(0, ni)
            def _(i):
                for s in range(STEPS):
                    for j in range(nj):
                        edges[s, side, i, j] = jnp.zeros((1, levels), jnp.float32)

    @pl.when(jnp.logical_and(even, at["lat"] < last))
    def _():
        pl.semaphore_wait(go_sem, 1)

    for side in (0, 1):
        pl.when(jnp.logical_and(even, has("lev", side)))(functools.partial(let_go, there("lev", side)))

    def send_lev(s, m):
        for side in (0, 1):
            @pl.when(has("lev", side))
            def _():
                for a in starts(m):
                    lev_copy(s, a, rows, m, side).start()

    load_t.wait()

    @pl.loop(0, chunks)
    def _(m):
        @pl.loop(0, rows)
        def _(r):
            for a in starts(m):
                for j in range(nj):
                    faces[0, 0, a + r, j] = t[0, 1 + j, 1 + a + r, 0:1]
                    faces[0, 1, a + r, j] = t[0, 1 + j, 1 + a + r, nk - 1:nk]

    @pl.when(odd)
    def _():
        pl.semaphore_wait(go_sem, count("lev"))

    @pl.loop(0, chunks)
    def _(m):
        send_lev(0, m)

    load_c.wait()

    below = lax.broadcasted_iota(jnp.int32, (nk, levels), 0) == 0
    above = lax.broadcasted_iota(jnp.int32, (nk, levels), 0) == nk - 1

    def stepped(s, i):
        for j in range(nj):
            middle = t[s, 1 + j, 1 + i]
            lower = jnp.where(below, edges[s, 0, i, j], pltpu.roll(middle, 1, 0))
            upper = jnp.where(above, edges[s, 1, i, j], pltpu.roll(middle, nk - 1, 0))
            spread = (t[s, j, 1 + i] + t[s, 2 + j, 1 + i] + t[s, 1 + j, i] + t[s, 1 + j, 2 + i]
                      + lower + upper - 6.0 * middle)
            yield j, middle + 0.1 * spread + 0.2 * middle * (1.0 - middle * c[j, i])

    def arrived(s, m):
        for side in (0, 1):
            @pl.when(has("lat", side))
            def _():
                lat_copy(s, 0, 2 * rows, m, 1 - side).wait_recv()

            @pl.when(has("lev", side))
            def _():
                lev_copy(s, 0, 2 * rows, m, 1 - side).wait_recv()

            @pl.when(jnp.logical_and(has("lon", side), m == 0))
            def _():
                lon_copy(s, 1 - side).wait_recv()

    @pl.loop(0, STEPS - 1)
    def _(s):
        @pl.loop(0, chunks)
        def _(m):
            arrived(s, m)

            @pl.loop(0, rows)
            def _(r):
                for a in starts(m):
                    for j, value in stepped(s, a + r):
                        t[s + 1, 1 + j, 1 + a + r] = value
                        faces[s + 1, 0, a + r, j] = value[0:1]
                        faces[s + 1, 1, a + r, j] = value[nk - 1:nk]

            for side in (0, 1):
                @pl.when(has("lat", side))
                def _():
                    for a in starts(m):
                        lat_copy(s + 1, a, rows, m, side).start()
            send_lev(s + 1, m)
            for side in (0, 1):
                @pl.when(jnp.logical_and(has("lon", side), m == 0))
                def _():
                    lon_copy(s + 1, side).start()

    def block(n):
        return pl.when(at["lat"] == n)

    @pl.loop(0, chunks)
    def _(m):
        arrived(STEPS - 1, m)

        @pl.loop(0, rows)
        def _(r):
            for a in starts(m):
                summed = None
                for j, value in stepped(STEPS - 1, a + r):
                    end[j, a + r] = value
                    summed = value if j == 0 else summed + value
                total[a + r] = summed

        for n in range(2 * half):
            p = 2 * half * m + n

            up = jnp.logical_or(jnp.logical_and(at["lat"] == 0, p >= CHAIN),
                                jnp.logical_and(at["lat"] == 2, p < SPLIT))
            down = jnp.logical_or(jnp.logical_and(at["lat"] == 1, p < SPLIT),
                                  jnp.logical_and(at["lat"] == 2, jnp.logical_and(p >= SPLIT, p < CHAIN)))

            @pl.when(up)
            def _():
                carry_copy(p).start()

            @pl.when(down)
            def _():
                suffix_copy(p, total).start()

    def combine(p, target, value):
        for r in range(piece):
            i = span(p).start + r
            target[i] = value(i)

    def add_suffix(p):
        suffix_copy(p, suffix).wait_recv()
        combine(p, suffix, lambda i: suffix[i] + total[i])

    def pass_up(p):
        carry_copy(p).wait_recv()
        combine(p, total, lambda i: total[i] + carried[i])
        carry_copy(p).start()

    @block(0)
    def _():
        @pl.loop(ROUND, CHAIN)
        def _(p):
            carry_copy(p).start()

        @pl.loop(RETURNED, ROUND)
        def _(p):
            carry_copy(p).start()

        @pl.loop(0, CHAIN)
        def _(p):
            add_suffix(p)
            round_copy(p).start()

    @block(1)
    def _():
        @pl.loop(SPLIT, CHAIN)
        def _(p):
            add_suffix(p)
            suffix_copy(p, suffix).start()
            pass_up(CHAIN - SPLIT + p)

        @pl.loop(2 * CHAIN - SPLIT, pieces)
        def _(p):
            pass_up(p)

        @pl.loop(ROUND, CHAIN)
        def _(p):
            pass_up(p)

        @pl.loop(0, SPLIT)
        def _(p):
            whole_copy(p).wait_recv()
            combine(p, carried, lambda i: whole[i] - total[i])

        @pl.loop(SPLIT, RETURNED)
        def _(p):
            whole_copy(p).wait_recv()
            combine(p, carried, lambda i: whole[i] - suffix[i])

        @pl.loop(RETURNED, ROUND)
        def _(p):
            carry_copy(p).wait_recv()

    @block(2)
    def _():
        paired = pieces - CHAIN - LEAD

        def take_whole(p):
            whole_copy(p).wait_recv()

            @pl.when(p < RETURNED)
            def _():
                whole_copy(p).start()

            @pl.when(p < SPLIT)
            def _():
                combine(p, carried, lambda i: whole[i])

            @pl.when(p >= SPLIT)
            def _():
                combine(p, carried, lambda i: whole[i] - total[i])

        @pl.loop(CHAIN, CHAIN + LEAD)
        def _(p):
            pass_up(p)

        @pl.loop(0, paired)
        def _(p):
            pass_up(CHAIN + LEAD + p)
            take_whole(p)

        @pl.loop(paired, ROUND)
        def _(p):
            take_whole(p)

        @pl.loop(ROUND, CHAIN)
        def _(p):
            carry_copy(p).wait_recv()

    @block(3)
    def _():
        @pl.loop(0, SPLIT)
        def _(p):
            whole_copy(p).wait_recv()
            whole_copy(p).start()
            carry_copy(p).wait_recv()
            combine(p, carried, lambda i: carried[i] + whole[i])

        @pl.loop(SPLIT, CHAIN)
        def _(p):
            whole_copy(p).wait_recv()

            @pl.when(p < ROUND)
            def _():
                whole_copy(p).start()
            combine(p, carried, lambda i: whole[i])

        @pl.loop(CHAIN, pieces)
        def _(p):
            carry_copy(p).wait_recv()

    for side in (0, 1):
        @pl.when(has("lat", side))
        def _():
            for s in range(STEPS):
                lat_copy(s, 0, ni, 0, side).wait_send()

        @pl.when(has("lon", side))
        def _():
            for s in range(STEPS):
                lon_copy(s, side).wait_send()

        @pl.when(has("lev", side))
        def _():
            for s in range(STEPS):
                lev_copy(s, 0, ni, 0, side).wait_send()

    chain = pieces - CHAIN

    @block(0)
    def _():
        carry_copy(0, chain + CHAIN - RETURNED).wait_send()
        round_copy(0, CHAIN).wait_send()

    @block(1)
    def _():
        carry_copy(0, chain + CHAIN - ROUND).wait_send()
        suffix_copy(0, suffix, CHAIN).wait_send()

    @block(2)
    def _():
        carry_copy(0, chain + SPLIT).wait_send()
        suffix_copy(0, total, CHAIN - SPLIT).wait_send()
        whole_copy(0, RETURNED).wait_send()

    @block(3)
    def _():
        whole_copy(0, ROUND).wait_send()


def march(tracer, crowding, rows):
    nj, ni, nk, levels = tracer.shape
    chunks = ni // (2 * rows)
    f32 = jnp.float32
    dma = pltpu.SemaphoreType.DMA
    return pl.pallas_call(
        functools.partial(march_kernel, rows),
        out_shape=(jax.ShapeDtypeStruct(tracer.shape, f32), jax.ShapeDtypeStruct(tracer.shape[1:], f32)),
        in_specs=[pl.BlockSpec(memory_space=pl.ANY)] * 2,
        out_specs=(pl.BlockSpec(memory_space=pltpu.VMEM),) * 2,
        scratch_shapes=[
            pltpu.VMEM((STEPS, nj + 2, ni + 2, nk, levels), f32),
            pltpu.VMEM((nj, ni, nk, levels), f32),
            pltpu.VMEM((STEPS, 2, ni, nj, 1, levels), f32),
            pltpu.VMEM((STEPS, 2, ni, nj, 1, levels), f32),
            pltpu.VMEM((ni, nk, levels), f32),
            pltpu.VMEM((ni, nk, levels), f32),
            pltpu.VMEM((ni, nk, levels), f32),
            dma((2,)),
            dma((10,)),
            dma((STEPS, chunks, 2)),
            dma((STEPS, 2)),
            dma((STEPS, chunks, 2)),
            dma((ni // min(PIECE, rows),)),
            dma((CHAIN,)),
            dma((CHAIN,)),
            pltpu.SemaphoreType.REGULAR,
        ],
        compiler_params=pltpu.CompilerParams(
            collective_id=0, has_side_effects=True, vmem_limit_bytes=48 * 2**20),
        name="march",
    )(tracer, crowding)


def sums_kernel(scale, block, end, carried, sums, copied, held, sem):
    nj, ni = end.shape[:2]
    blocks = ni // block

    def written(n, b):
        at_b = pl.ds(b * block, block)
        source, target = ((end, copied), (held, sums))[n]
        return pltpu.make_async_copy(source.at[:, at_b], target.at[:, at_b], sem.at[n, b])

    for b in range(blocks):
        written(0, b).start()
    for b in range(blocks):
        @pl.loop(b * block, (b + 1) * block)
        def _(i):
            run = carried[i]
            for j in range(nj):
                run = run + end[j, i]
                held[j, i] = run * scale
        written(1, b).start()
    for b in range(blocks):
        for n in (0, 1):
            written(n, b).wait()


def sums_along_j(end, carried, cells):
    ni = end.shape[1]
    block = min(8, ni)
    return pl.pallas_call(
        functools.partial(sums_kernel, 1.0 / cells, block),
        out_shape=(jax.ShapeDtypeStruct(end.shape, end.dtype),) * 2,
        in_specs=[pl.BlockSpec(memory_space=pltpu.VMEM)] * 2,
        out_specs=(pl.BlockSpec(memory_space=pl.ANY),) * 2,
        scratch_shapes=[pltpu.VMEM(end.shape, end.dtype), pltpu.SemaphoreType.DMA((2, ni // block))],
        compiler_params=pltpu.CompilerParams(vmem_limit_bytes=12 * 2**20),
        name="sums",
    )(end, carried)


def on_device(tracer, crowding):
    end, carried = march(tracer, crowding, min(ROWS, tracer.shape[1] // 2))
    return sums_along_j(end, carried, tracer.shape[0] * lax.axis_size("lat"))


def solution(mesh):
    spec = P(("unit", "lat"), "lon", "lev", None)
    return jax.shard_map(
        on_device, mesh=mesh, in_specs=(spec, spec), out_specs=(spec, spec), check_vma=False)
```

```python
import functools

import jax
import jax.numpy as jnp
from jax import lax
from jax.experimental import pallas as pl
from jax.experimental.pallas import tpu as pltpu
from jax.sharding import PartitionSpec as P

STEPS = 4
ROWS = 8
PIECE = 2
SPLIT = 8
ROUND = 14
CHAIN = 19
RETURNED = 9
LEAD = 4
MESH = pl.DeviceIdType.MESH
AXES = ("unit", "lat", "lon", "lev")


def march_kernel(rows, tracer, crowding, end, carried, t, c, faces, edges, total, suffix, whole,
                 load_sem, send_sem, lat_sem, lon_sem, lev_sem, carry_sem, suffix_sem, whole_sem,
                 go_sem):
    nj, ni, nk, levels = tracer.shape
    chunks = ni // (2 * rows)
    at = {axis: lax.axis_index(axis) for axis in AXES}
    size = {axis: lax.axis_size(axis) for axis in AXES}

    def has(axis, side):
        return at[axis] > 0 if side == 0 else at[axis] < size[axis] - 1

    def there(axis, side):
        return {axis: at[axis] - 1 if side == 0 else at[axis] + 1}

    def starts(m):
        return (m * rows, ni - (m + 1) * rows)

    def lat_copy(s, a, length, m, side, source=None):
        row = 0 if side == 0 else nj - 1
        if source is None:
            source = t.at[s, 1 + row, pl.ds(1 + a, length)]
        return pltpu.make_async_remote_copy(
            source, t.at[s, nj + 1 if side == 0 else 0, pl.ds(1 + a, length)],
            send_sem.at[side], lat_sem.at[s, m, 1 - side], device_id=there("lat", side), device_id_type=MESH)

    def lon_copy(s, side, source=None):
        if source is None:
            source = t.at[s, pl.ds(1, nj), 1 if side == 0 else ni]
        return pltpu.make_async_remote_copy(
            source, t.at[s, pl.ds(1, nj), ni + 1 if side == 0 else 0],
            send_sem.at[2 + side], lon_sem.at[s, 1 - side], device_id=there("lon", side), device_id_type=MESH)

    def lev_copy(s, a, length, m, side):
        return pltpu.make_async_remote_copy(
            faces.at[s, side, pl.ds(a, length)], edges.at[s, 1 - side, pl.ds(a, length)],
            send_sem.at[4 + side], lev_sem.at[s, m, 1 - side], device_id=there("lev", side), device_id_type=MESH)

    piece = min(PIECE, rows)
    half = rows // piece
    pieces = 2 * half * chunks
    assert CHAIN - SPLIT <= pieces - CHAIN <= ROUND + LEAD
    last = size["lat"] - 1

    def span(p):
        m, n = p // (2 * half), p % (2 * half)
        if isinstance(p, int):
            return pl.ds((m * rows if n < half else ni - (m + 1) * rows - rows) + n * piece, piece)
        start = jnp.where(n < half, m * rows, ni - (m + 1) * rows - rows)
        return pl.ds(start + n * piece, piece)

    def carry_copy(p, count=1):
        at_p = span(p) if count == 1 else pl.ds(0, count * piece)
        return pltpu.make_async_remote_copy(
            total.at[at_p], carried.at[at_p], send_sem.at[6], carry_sem.at[p],
            device_id=there("lat", 1), device_id_type=MESH)

    def suffix_copy(p, source, count=1):
        at_p = span(p) if count == 1 else pl.ds(0, count * piece)
        return pltpu.make_async_remote_copy(
            source.at[at_p], suffix.at[at_p], send_sem.at[7], suffix_sem.at[p],
            device_id=there("lat", 0), device_id_type=MESH)

    def round_copy(p, count=1):
        at_p = span(p) if count == 1 else pl.ds(0, count * piece)
        return pltpu.make_async_remote_copy(
            suffix.at[at_p], whole.at[at_p], send_sem.at[8], whole_sem.at[p],
            device_id={"lat": last}, device_id_type=MESH)

    def whole_copy(p, count=1):
        at_p = span(p) if count == 1 else pl.ds(0, count * piece)
        return pltpu.make_async_remote_copy(
            whole.at[at_p], whole.at[at_p], send_sem.at[9], whole_sem.at[p],
            device_id=there("lat", 0), device_id_type=MESH)

    load_t = pltpu.make_async_copy(tracer, t.at[0, pl.ds(1, nj), pl.ds(1, ni)], load_sem.at[0])
    load_c = pltpu.make_async_copy(crowding, c, load_sem.at[1])

    barrier = pltpu.get_barrier_semaphore()

    def greet(where):
        pl.semaphore_signal(barrier, inc=1, device_id=where, device_id_type=MESH)

    def let_go(where):
        pl.semaphore_signal(go_sem, inc=1, device_id=where, device_id_type=MESH)

    def count(axis):
        return has(axis, 0).astype(jnp.int32) + has(axis, 1).astype(jnp.int32)

    odd = at["lev"] % 2 == 1
    even = at["lev"] % 2 == 0
    keeper = jnp.logical_and(even, at["lat"] == last)
    ends = jnp.logical_or(at["lat"] == 0, at["lat"] == last)
    between = jnp.logical_and(at["lat"] > 0, at["lat"] < last - 1)
    for axis in ("lat", "lon"):
        for side in (0, 1):
            pl.when(has(axis, side))(functools.partial(greet, there(axis, side)))
    pl.when(ends)(functools.partial(greet, {"lat": last - at["lat"]}))
    pl.when(jnp.logical_and(even, between))(functools.partial(greet, {"lat": last}))
    load_t.start()
    load_c.start()

    near = count("lat") + count("lon") + ends.astype(jnp.int32)
    pl.semaphore_wait(
        barrier, near + jnp.where(keeper, last - 2 + size["lat"] * count("lev"), 0))
    for side in (0, 1):
        pl.when(jnp.logical_and(odd, has("lev", side)))(
            functools.partial(greet, {"lat": last, **there("lev", side)}))

    for m in range(chunks):
        for side in (0, 1):
            @pl.when(has("lat", side))
            def _():
                for a in starts(m):
                    lat_copy(0, a, rows, m, side,
                             tracer.at[0 if side == 0 else nj - 1, pl.ds(a, rows)]).start()
    for side in (0, 1):
        @pl.when(has("lon", side))
        def _():
            lon_copy(0, side, tracer.at[:, 0 if side == 0 else ni - 1]).start()

    @pl.when(keeper)
    def _():
        for n in range(last):
            let_go({"lat": n})

    zero = jnp.zeros((nk, levels), jnp.float32)
    for side in (0, 1):
        @pl.when(jnp.logical_not(has("lat", side)))
        def _():
            @pl.loop(0, ni)
            def _(i):
                for s in range(STEPS):
                    t[s, 0 if side == 0 else nj + 1, 1 + i] = zero

            if side == 0:
                @pl.loop(0, ni)
                def _(i):
                    carried[i] = zero

        @pl.when(jnp.logical_not(has("lon", side)))
        def _():
            for s in range(STEPS):
                for j in range(nj):
                    t[s, 1 + j, 0 if side == 0 else ni + 1] = zero

        @pl.when(jnp.logical_not(has("lev", side)))
        def _():
            @pl.loop(0, ni)
            def _(i):
                for s in range(STEPS):
                    for j in range(nj):
                        edges[s, side, i, j] = jnp.zeros((1, levels), jnp.float32)

    @pl.when(jnp.logical_and(even, at["lat"] < last))
    def _():
        pl.semaphore_wait(go_sem, 1)

    for side in (0, 1):
        pl.when(jnp.logical_and(even, has("lev", side)))(functools.partial(let_go, there("lev", side)))

    def send_lev(s, m):
        for side in (0, 1):
            @pl.when(has("lev", side))
            def _():
                for a in starts(m):
                    lev_copy(s, a, rows, m, side).start()

    load_t.wait()

    @pl.loop(0, chunks)
    def _(m):
        @pl.loop(0, rows)
        def _(r):
            for a in starts(m):
                for j in range(nj):
                    faces[0, 0, a + r, j] = t[0, 1 + j, 1 + a + r, 0:1]
                    faces[0, 1, a + r, j] = t[0, 1 + j, 1 + a + r, nk - 1:nk]

    @pl.when(odd)
    def _():
        pl.semaphore_wait(go_sem, count("lev"))

    @pl.loop(0, chunks)
    def _(m):
        send_lev(0, m)

    load_c.wait()

    below = lax.broadcasted_iota(jnp.int32, (nk, levels), 0) == 0
    above = lax.broadcasted_iota(jnp.int32, (nk, levels), 0) == nk - 1

    def stepped(s, i):
        for j in range(nj):
            middle = t[s, 1 + j, 1 + i]
            lower = jnp.where(below, edges[s, 0, i, j], pltpu.roll(middle, 1, 0))
            upper = jnp.where(above, edges[s, 1, i, j], pltpu.roll(middle, nk - 1, 0))
            spread = (t[s, j, 1 + i] + t[s, 2 + j, 1 + i] + t[s, 1 + j, i] + t[s, 1 + j, 2 + i]
                      + lower + upper - 6.0 * middle)
            yield j, middle + 0.1 * spread + 0.2 * middle * (1.0 - middle * c[j, i])

    def arrived(s, m):
        for side in (0, 1):
            @pl.when(has("lat", side))
            def _():
                lat_copy(s, 0, 2 * rows, m, 1 - side).wait_recv()

            @pl.when(has("lev", side))
            def _():
                lev_copy(s, 0, 2 * rows, m, 1 - side).wait_recv()

            @pl.when(jnp.logical_and(has("lon", side), m == 0))
            def _():
                lon_copy(s, 1 - side).wait_recv()

    @pl.loop(0, STEPS - 1)
    def _(s):
        @pl.loop(0, chunks)
        def _(m):
            arrived(s, m)

            @pl.loop(0, rows)
            def _(r):
                for a in starts(m):
                    for j, value in stepped(s, a + r):
                        t[s + 1, 1 + j, 1 + a + r] = value
                        faces[s + 1, 0, a + r, j] = value[0:1]
                        faces[s + 1, 1, a + r, j] = value[nk - 1:nk]

            for side in (0, 1):
                @pl.when(has("lat", side))
                def _():
                    for a in starts(m):
                        lat_copy(s + 1, a, rows, m, side).start()
            send_lev(s + 1, m)
            for side in (0, 1):
                @pl.when(jnp.logical_and(has("lon", side), m == 0))
                def _():
                    lon_copy(s + 1, side).start()

    def block(n):
        return pl.when(at["lat"] == n)

    @pl.loop(0, chunks)
    def _(m):
        arrived(STEPS - 1, m)

        @pl.loop(0, rows)
        def _(r):
            for a in starts(m):
                summed = None
                for j, value in stepped(STEPS - 1, a + r):
                    end[j, a + r] = value
                    summed = value if j == 0 else summed + value
                total[a + r] = summed

        for n in range(2 * half):
            p = 2 * half * m + n

            up = jnp.logical_or(jnp.logical_and(at["lat"] == 0, p >= CHAIN),
                                jnp.logical_and(at["lat"] == 2, p < SPLIT))
            down = jnp.logical_or(jnp.logical_and(at["lat"] == 1, p < SPLIT),
                                  jnp.logical_and(at["lat"] == 2, jnp.logical_and(p >= SPLIT, p < CHAIN)))

            @pl.when(up)
            def _():
                carry_copy(p).start()

            @pl.when(down)
            def _():
                suffix_copy(p, total).start()

    def combine(p, target, value):
        for r in range(piece):
            i = span(p).start + r
            target[i] = value(i)

    def add_suffix(p):
        suffix_copy(p, suffix).wait_recv()
        combine(p, suffix, lambda i: suffix[i] + total[i])

    def pass_up(p):
        carry_copy(p).wait_recv()
        combine(p, total, lambda i: total[i] + carried[i])
        carry_copy(p).start()

    def unrolled(start, stop):
        def run(body):
            for p in range(start, stop):
                body(p)
        return run

    @block(0)
    def _():
        @unrolled(ROUND, CHAIN)
        def _(p):
            carry_copy(p).start()

        @unrolled(RETURNED, ROUND)
        def _(p):
            carry_copy(p).start()

        @unrolled(0, CHAIN)
        def _(p):
            add_suffix(p)
            round_copy(p).start()

    @block(1)
    def _():
        @unrolled(SPLIT, CHAIN)
        def _(p):
            pass_up(CHAIN - SPLIT + p)
            add_suffix(p)
            suffix_copy(p, suffix).start()

        @unrolled(2 * CHAIN - SPLIT, pieces)
        def _(p):
            pass_up(p)

        @unrolled(ROUND, CHAIN)
        def _(p):
            pass_up(p)

        @unrolled(0, SPLIT)
        def _(p):
            whole_copy(p).wait_recv()
            combine(p, carried, lambda i: whole[i] - total[i])

        @unrolled(SPLIT, RETURNED)
        def _(p):
            whole_copy(p).wait_recv()
            combine(p, carried, lambda i: whole[i] - suffix[i])

        @unrolled(RETURNED, ROUND)
        def _(p):
            carry_copy(p).wait_recv()

    @block(2)
    def _():
        paired = pieces - CHAIN - LEAD

        def take_whole(p):
            whole_copy(p).wait_recv()

            @pl.when(p < RETURNED)
            def _():
                whole_copy(p).start()

            @pl.when(p < SPLIT)
            def _():
                combine(p, carried, lambda i: whole[i])

            @pl.when(p >= SPLIT)
            def _():
                combine(p, carried, lambda i: whole[i] - total[i])

        @unrolled(CHAIN, CHAIN + LEAD)
        def _(p):
            pass_up(p)

        @unrolled(0, paired)
        def _(p):
            pass_up(CHAIN + LEAD + p)
            take_whole(p)

        @unrolled(paired, ROUND)
        def _(p):
            take_whole(p)

        @unrolled(ROUND, CHAIN)
        def _(p):
            carry_copy(p).wait_recv()

    @block(3)
    def _():
        @unrolled(0, SPLIT)
        def _(p):
            whole_copy(p).wait_recv()
            whole_copy(p).start()
            carry_copy(p).wait_recv()
            combine(p, carried, lambda i: carried[i] + whole[i])

        @unrolled(SPLIT, CHAIN)
        def _(p):
            whole_copy(p).wait_recv()

            @pl.when(p < ROUND)
            def _():
                whole_copy(p).start()
            combine(p, carried, lambda i: whole[i])

        @unrolled(CHAIN, pieces)
        def _(p):
            carry_copy(p).wait_recv()

    for side in (0, 1):
        @pl.when(has("lat", side))
        def _():
            for s in range(STEPS):
                lat_copy(s, 0, ni, 0, side).wait_send()

        @pl.when(has("lon", side))
        def _():
            for s in range(STEPS):
                lon_copy(s, side).wait_send()

        @pl.when(has("lev", side))
        def _():
            for s in range(STEPS):
                lev_copy(s, 0, ni, 0, side).wait_send()

    chain = pieces - CHAIN

    @block(0)
    def _():
        carry_copy(0, chain + CHAIN - RETURNED).wait_send()
        round_copy(0, CHAIN).wait_send()

    @block(1)
    def _():
        carry_copy(0, chain + CHAIN - ROUND).wait_send()
        suffix_copy(0, suffix, CHAIN).wait_send()

    @block(2)
    def _():
        carry_copy(0, chain + SPLIT).wait_send()
        suffix_copy(0, total, CHAIN - SPLIT).wait_send()
        whole_copy(0, RETURNED).wait_send()

    @block(3)
    def _():
        whole_copy(0, ROUND).wait_send()


def march(tracer, crowding, rows):
    nj, ni, nk, levels = tracer.shape
    chunks = ni // (2 * rows)
    f32 = jnp.float32
    dma = pltpu.SemaphoreType.DMA
    return pl.pallas_call(
        functools.partial(march_kernel, rows),
        out_shape=(jax.ShapeDtypeStruct(tracer.shape, f32), jax.ShapeDtypeStruct(tracer.shape[1:], f32)),
        in_specs=[pl.BlockSpec(memory_space=pl.ANY)] * 2,
        out_specs=(pl.BlockSpec(memory_space=pltpu.VMEM),) * 2,
        scratch_shapes=[
            pltpu.VMEM((STEPS, nj + 2, ni + 2, nk, levels), f32),
            pltpu.VMEM((nj, ni, nk, levels), f32),
            pltpu.VMEM((STEPS, 2, ni, nj, 1, levels), f32),
            pltpu.VMEM((STEPS, 2, ni, nj, 1, levels), f32),
            pltpu.VMEM((ni, nk, levels), f32),
            pltpu.VMEM((ni, nk, levels), f32),
            pltpu.VMEM((ni, nk, levels), f32),
            dma((2,)),
            dma((10,)),
            dma((STEPS, chunks, 2)),
            dma((STEPS, 2)),
            dma((STEPS, chunks, 2)),
            dma((ni // min(PIECE, rows),)),
            dma((CHAIN,)),
            dma((CHAIN,)),
            pltpu.SemaphoreType.REGULAR,
        ],
        compiler_params=pltpu.CompilerParams(
            collective_id=0, has_side_effects=True, vmem_limit_bytes=48 * 2**20),
        name="march",
    )(tracer, crowding)


def sums_kernel(scale, block, end, carried, sums, copied, held, sem):
    nj, ni = end.shape[:2]
    blocks = ni // block

    def written(n, b):
        at_b = pl.ds(b * block, block)
        source, target = ((end, copied), (held, sums))[n]
        return pltpu.make_async_copy(source.at[:, at_b], target.at[:, at_b], sem.at[n, b])

    for b in range(blocks):
        written(0, b).start()
    for b in range(blocks):
        @pl.loop(b * block, (b + 1) * block)
        def _(i):
            run = carried[i]
            for j in range(nj):
                run = run + end[j, i]
                held[j, i] = run * scale
        written(1, b).start()
    for b in range(blocks):
        for n in (0, 1):
            written(n, b).wait()


def sums_along_j(end, carried, cells):
    ni = end.shape[1]
    block = min(8, ni)
    return pl.pallas_call(
        functools.partial(sums_kernel, 1.0 / cells, block),
        out_shape=(jax.ShapeDtypeStruct(end.shape, end.dtype),) * 2,
        in_specs=[pl.BlockSpec(memory_space=pltpu.VMEM)] * 2,
        out_specs=(pl.BlockSpec(memory_space=pl.ANY),) * 2,
        scratch_shapes=[pltpu.VMEM(end.shape, end.dtype), pltpu.SemaphoreType.DMA((2, ni // block))],
        compiler_params=pltpu.CompilerParams(vmem_limit_bytes=12 * 2**20),
        name="sums",
    )(end, carried)


def on_device(tracer, crowding):
    end, carried = march(tracer, crowding, min(ROWS, tracer.shape[1] // 2))
    return sums_along_j(end, carried, tracer.shape[0] * lax.axis_size("lat"))


def solution(mesh):
    spec = P(("unit", "lat"), "lon", "lev", None)
    return jax.shard_map(
        on_device, mesh=mesh, in_specs=(spec, spec), out_specs=(spec, spec), check_vma=False)
```

```python
import functools

import jax
import jax.numpy as jnp
from jax import lax
from jax.experimental import pallas as pl
from jax.experimental.pallas import tpu as pltpu
from jax.sharding import PartitionSpec as P

STEPS = 4
ROWS = 8
PIECE = 2
SPLIT = 8
ROUND = 14
CHAIN = 19
RETURNED = 9
LEAD = 4
MESH = pl.DeviceIdType.MESH
AXES = ("unit", "lat", "lon", "lev")


def march_kernel(rows, tracer, crowding, end, carried, t, c, faces, edges, total, suffix, whole,
                 load_sem, send_sem, lat_sem, lon_sem, lev_sem, carry_sem, suffix_sem, whole_sem,
                 go_sem):
    nj, ni, nk, levels = tracer.shape
    chunks = ni // (2 * rows)
    at = {axis: lax.axis_index(axis) for axis in AXES}
    size = {axis: lax.axis_size(axis) for axis in AXES}

    def has(axis, side):
        return at[axis] > 0 if side == 0 else at[axis] < size[axis] - 1

    def there(axis, side):
        return {axis: lax.rem(at[axis] + (size[axis] - 1 if side == 0 else 1), size[axis])}

    def starts(m):
        return (m * rows, ni - (m + 1) * rows)

    def lat_copy(s, a, length, m, side, source=None):
        row = 0 if side == 0 else nj - 1
        if source is None:
            source = t.at[s, 1 + row, pl.ds(1 + a, length)]
        return pltpu.make_async_remote_copy(
            source, t.at[s, nj + 1 if side == 0 else 0, pl.ds(1 + a, length)],
            send_sem.at[side], lat_sem.at[s, m, 1 - side], device_id=there("lat", side), device_id_type=MESH)

    def lon_copy(s, side, source=None):
        if source is None:
            source = t.at[s, pl.ds(1, nj), 1 if side == 0 else ni]
        return pltpu.make_async_remote_copy(
            source, t.at[s, pl.ds(1, nj), ni + 1 if side == 0 else 0],
            send_sem.at[2 + side], lon_sem.at[s, 1 - side], device_id=there("lon", side), device_id_type=MESH)

    def lev_copy(s, a, length, m, side):
        return pltpu.make_async_remote_copy(
            faces.at[s, side, pl.ds(a, length)], edges.at[s, 1 - side, pl.ds(a, length)],
            send_sem.at[4 + side], lev_sem.at[s, m, 1 - side], device_id=there("lev", side), device_id_type=MESH)

    piece = min(PIECE, rows)
    half = rows // piece
    pieces = 2 * half * chunks
    assert CHAIN - SPLIT <= pieces - CHAIN <= ROUND + LEAD
    last = size["lat"] - 1

    def span(p):
        m, n = p // (2 * half), p % (2 * half)
        if isinstance(p, int):
            return pl.ds((m * rows if n < half else ni - (m + 1) * rows - rows) + n * piece, piece)
        start = jnp.where(n < half, m * rows, ni - (m + 1) * rows - rows)
        return pl.ds(start + n * piece, piece)

    def carry_copy(p, count=1):
        at_p = span(p) if count == 1 else pl.ds(0, count * piece)
        return pltpu.make_async_remote_copy(
            total.at[at_p], carried.at[at_p], send_sem.at[6], carry_sem.at[p],
            device_id=there("lat", 1), device_id_type=MESH)

    def suffix_copy(p, source, count=1):
        at_p = span(p) if count == 1 else pl.ds(0, count * piece)
        return pltpu.make_async_remote_copy(
            source.at[at_p], suffix.at[at_p], send_sem.at[7], suffix_sem.at[p],
            device_id=there("lat", 0), device_id_type=MESH)

    def round_copy(p, count=1):
        at_p = span(p) if count == 1 else pl.ds(0, count * piece)
        return pltpu.make_async_remote_copy(
            suffix.at[at_p], whole.at[at_p], send_sem.at[8], whole_sem.at[p],
            device_id={"lat": last}, device_id_type=MESH)

    def whole_copy(p, count=1):
        at_p = span(p) if count == 1 else pl.ds(0, count * piece)
        return pltpu.make_async_remote_copy(
            whole.at[at_p], whole.at[at_p], send_sem.at[9], whole_sem.at[p],
            device_id=there("lat", 0), device_id_type=MESH)

    load_t = pltpu.make_async_copy(tracer, t.at[0, pl.ds(1, nj), pl.ds(1, ni)], load_sem.at[0])
    load_c = pltpu.make_async_copy(crowding, c, load_sem.at[1])

    barrier = pltpu.get_barrier_semaphore()

    def greet(where):
        pl.semaphore_signal(barrier, inc=1, device_id=where, device_id_type=MESH)

    def let_go(where):
        pl.semaphore_signal(go_sem, inc=1, device_id=where, device_id_type=MESH)

    def count(axis):
        return has(axis, 0).astype(jnp.int32) + has(axis, 1).astype(jnp.int32)

    odd = at["lev"] % 2 == 1
    even = at["lev"] % 2 == 0
    keeper = jnp.logical_and(even, at["lat"] == last)
    ends = jnp.logical_or(at["lat"] == 0, at["lat"] == last)
    between = jnp.logical_and(at["lat"] > 0, at["lat"] < last - 1)
    for axis in ("lat", "lon"):
        for side in (0, 1):
            pl.when(has(axis, side))(functools.partial(greet, there(axis, side)))
    pl.when(ends)(functools.partial(greet, {"lat": last - at["lat"]}))
    pl.when(jnp.logical_and(even, between))(functools.partial(greet, {"lat": last}))
    load_t.start()
    load_c.start()

    near = count("lat") + count("lon") + ends.astype(jnp.int32)
    pl.semaphore_wait(
        barrier, near + jnp.where(keeper, last - 2 + size["lat"] * count("lev"), 0))
    for side in (0, 1):
        pl.when(jnp.logical_and(odd, has("lev", side)))(
            functools.partial(greet, {"lat": last, **there("lev", side)}))

    for m in range(chunks):
        for side in (0, 1):
            @pl.when(has("lat", side))
            def _():
                for a in starts(m):
                    lat_copy(0, a, rows, m, side,
                             tracer.at[0 if side == 0 else nj - 1, pl.ds(a, rows)]).start()
    for side in (0, 1):
        @pl.when(has("lon", side))
        def _():
            lon_copy(0, side, tracer.at[:, 0 if side == 0 else ni - 1]).start()

    @pl.when(keeper)
    def _():
        for n in range(last):
            let_go({"lat": n})

    zero = jnp.zeros((nk, levels), jnp.float32)
    for side in (0, 1):
        @pl.when(jnp.logical_not(has("lat", side)))
        def _():
            @pl.loop(0, ni)
            def _(i):
                for s in range(STEPS):
                    t[s, 0 if side == 0 else nj + 1, 1 + i] = zero

            if side == 0:
                @pl.loop(0, ni)
                def _(i):
                    carried[i] = zero

        @pl.when(jnp.logical_not(has("lon", side)))
        def _():
            for s in range(STEPS):
                for j in range(nj):
                    t[s, 1 + j, 0 if side == 0 else ni + 1] = zero

        @pl.when(jnp.logical_not(has("lev", side)))
        def _():
            @pl.loop(0, ni)
            def _(i):
                for s in range(STEPS):
                    for j in range(nj):
                        edges[s, side, i, j] = jnp.zeros((1, levels), jnp.float32)

    @pl.when(jnp.logical_and(even, at["lat"] < last))
    def _():
        pl.semaphore_wait(go_sem, 1)

    for side in (0, 1):
        pl.when(jnp.logical_and(even, has("lev", side)))(functools.partial(let_go, there("lev", side)))

    def send_lev(s, m):
        for side in (0, 1):
            @pl.when(has("lev", side))
            def _():
                for a in starts(m):
                    lev_copy(s, a, rows, m, side).start()

    load_t.wait()

    @pl.loop(0, chunks)
    def _(m):
        @pl.loop(0, rows)
        def _(r):
            for a in starts(m):
                for j in range(nj):
                    faces[0, 0, a + r, j] = t[0, 1 + j, 1 + a + r, 0:1]
                    faces[0, 1, a + r, j] = t[0, 1 + j, 1 + a + r, nk - 1:nk]

    @pl.when(odd)
    def _():
        pl.semaphore_wait(go_sem, count("lev"))

    @pl.loop(0, chunks)
    def _(m):
        send_lev(0, m)

    load_c.wait()

    below = lax.broadcasted_iota(jnp.int32, (nk, levels), 0) == 0
    above = lax.broadcasted_iota(jnp.int32, (nk, levels), 0) == nk - 1

    def stepped(s, i):
        for j in range(nj):
            middle = t[s, 1 + j, 1 + i]
            lower = jnp.where(below, edges[s, 0, i, j], pltpu.roll(middle, 1, 0))
            upper = jnp.where(above, edges[s, 1, i, j], pltpu.roll(middle, nk - 1, 0))
            spread = (t[s, j, 1 + i] + t[s, 2 + j, 1 + i] + t[s, 1 + j, i] + t[s, 1 + j, 2 + i]
                      + lower + upper - 6.0 * middle)
            yield j, middle + 0.1 * spread + 0.2 * middle * (1.0 - middle * c[j, i])

    def arrived(s, m):
        for side in (0, 1):
            @pl.when(has("lat", side))
            def _():
                lat_copy(s, 0, 2 * rows, m, 1 - side).wait_recv()

            @pl.when(has("lev", side))
            def _():
                lev_copy(s, 0, 2 * rows, m, 1 - side).wait_recv()

            @pl.when(jnp.logical_and(has("lon", side), m == 0))
            def _():
                lon_copy(s, 1 - side).wait_recv()

    @pl.loop(0, STEPS - 1)
    def _(s):
        @pl.loop(0, chunks)
        def _(m):
            arrived(s, m)

            @pl.loop(0, rows)
            def _(r):
                for a in starts(m):
                    for j, value in stepped(s, a + r):
                        t[s + 1, 1 + j, 1 + a + r] = value
                        faces[s + 1, 0, a + r, j] = value[0:1]
                        faces[s + 1, 1, a + r, j] = value[nk - 1:nk]

            for side in (0, 1):
                @pl.when(has("lat", side))
                def _():
                    for a in starts(m):
                        lat_copy(s + 1, a, rows, m, side).start()
            send_lev(s + 1, m)
            for side in (0, 1):
                @pl.when(jnp.logical_and(has("lon", side), m == 0))
                def _():
                    lon_copy(s + 1, side).start()

    def block(n):
        return pl.when(at["lat"] == n)

    @pl.loop(0, chunks)
    def _(m):
        arrived(STEPS - 1, m)

        @pl.loop(0, rows)
        def _(r):
            for a in starts(m):
                summed = None
                for j, value in stepped(STEPS - 1, a + r):
                    end[j, a + r] = value
                    summed = value if j == 0 else summed + value
                total[a + r] = summed

        for n in range(2 * half):
            p = 2 * half * m + n

            up = jnp.logical_or(jnp.logical_and(at["lat"] == 0, p >= CHAIN),
                                jnp.logical_and(at["lat"] == 2, p < SPLIT))
            down = jnp.logical_or(jnp.logical_and(at["lat"] == 1, p < SPLIT),
                                  jnp.logical_and(at["lat"] == 2, jnp.logical_and(p >= SPLIT, p < CHAIN)))

            @pl.when(up)
            def _():
                carry_copy(p).start()

            @pl.when(down)
            def _():
                suffix_copy(p, total).start()

    def combine(p, target, value):
        for r in range(piece):
            i = span(p).start + r
            target[i] = value(i)

    def add_suffix(p):
        suffix_copy(p, suffix).wait_recv()
        combine(p, suffix, lambda i: suffix[i] + total[i])

    def pass_up(p):
        carry_copy(p).wait_recv()
        combine(p, total, lambda i: total[i] + carried[i])
        carry_copy(p).start()

    def unrolled(start, stop):
        def run(body):
            for p in range(start, stop):
                body(p)
        return run

    @block(0)
    def _():
        @unrolled(ROUND, CHAIN)
        def _(p):
            carry_copy(p).start()

        @unrolled(RETURNED, ROUND)
        def _(p):
            carry_copy(p).start()

        @unrolled(0, CHAIN)
        def _(p):
            add_suffix(p)
            round_copy(p).start()

    @block(1)
    def _():
        @unrolled(SPLIT, CHAIN)
        def _(p):
            pass_up(CHAIN - SPLIT + p)
            add_suffix(p)
            suffix_copy(p, suffix).start()

        @unrolled(2 * CHAIN - SPLIT, pieces)
        def _(p):
            pass_up(p)

        @unrolled(ROUND, CHAIN)
        def _(p):
            pass_up(p)

        @unrolled(0, SPLIT)
        def _(p):
            whole_copy(p).wait_recv()
            combine(p, carried, lambda i: whole[i] - total[i])

        @unrolled(SPLIT, RETURNED)
        def _(p):
            whole_copy(p).wait_recv()
            combine(p, carried, lambda i: whole[i] - suffix[i])

        @unrolled(RETURNED, ROUND)
        def _(p):
            carry_copy(p).wait_recv()

    @block(2)
    def _():
        paired = pieces - CHAIN - LEAD

        def take_whole(p):
            whole_copy(p).wait_recv()

            @pl.when(p < RETURNED)
            def _():
                whole_copy(p).start()

            @pl.when(p < SPLIT)
            def _():
                combine(p, carried, lambda i: whole[i])

            @pl.when(p >= SPLIT)
            def _():
                combine(p, carried, lambda i: whole[i] - total[i])

        @unrolled(CHAIN, CHAIN + LEAD)
        def _(p):
            pass_up(p)

        @unrolled(0, paired)
        def _(p):
            pass_up(CHAIN + LEAD + p)
            take_whole(p)

        @unrolled(paired, ROUND)
        def _(p):
            take_whole(p)

        @unrolled(ROUND, CHAIN)
        def _(p):
            carry_copy(p).wait_recv()

    @block(3)
    def _():
        @unrolled(0, SPLIT)
        def _(p):
            whole_copy(p).wait_recv()
            whole_copy(p).start()
            carry_copy(p).wait_recv()
            combine(p, carried, lambda i: carried[i] + whole[i])

        @unrolled(SPLIT, CHAIN)
        def _(p):
            whole_copy(p).wait_recv()

            @pl.when(p < ROUND)
            def _():
                whole_copy(p).start()
            combine(p, carried, lambda i: whole[i])

        @unrolled(CHAIN, pieces)
        def _(p):
            carry_copy(p).wait_recv()

    for side in (0, 1):
        @pl.when(has("lat", side))
        def _():
            for s in range(STEPS):
                lat_copy(s, 0, ni, 0, side).wait_send()

        @pl.when(has("lon", side))
        def _():
            for s in range(STEPS):
                lon_copy(s, side).wait_send()

        @pl.when(has("lev", side))
        def _():
            for s in range(STEPS):
                lev_copy(s, 0, ni, 0, side).wait_send()

    chain = pieces - CHAIN

    @block(0)
    def _():
        carry_copy(0, chain + CHAIN - RETURNED).wait_send()
        round_copy(0, CHAIN).wait_send()

    @block(1)
    def _():
        carry_copy(0, chain + CHAIN - ROUND).wait_send()
        suffix_copy(0, suffix, CHAIN).wait_send()

    @block(2)
    def _():
        carry_copy(0, chain + SPLIT).wait_send()
        suffix_copy(0, total, CHAIN - SPLIT).wait_send()
        whole_copy(0, RETURNED).wait_send()

    @block(3)
    def _():
        whole_copy(0, ROUND).wait_send()


def march(tracer, crowding, rows):
    nj, ni, nk, levels = tracer.shape
    chunks = ni // (2 * rows)
    f32 = jnp.float32
    dma = pltpu.SemaphoreType.DMA
    return pl.pallas_call(
        functools.partial(march_kernel, rows),
        out_shape=(jax.ShapeDtypeStruct(tracer.shape, f32), jax.ShapeDtypeStruct(tracer.shape[1:], f32)),
        in_specs=[pl.BlockSpec(memory_space=pl.ANY)] * 2,
        out_specs=(pl.BlockSpec(memory_space=pltpu.VMEM),) * 2,
        scratch_shapes=[
            pltpu.VMEM((STEPS, nj + 2, ni + 2, nk, levels), f32),
            pltpu.VMEM((nj, ni, nk, levels), f32),
            pltpu.VMEM((STEPS, 2, ni, nj, 1, levels), f32),
            pltpu.VMEM((STEPS, 2, ni, nj, 1, levels), f32),
            pltpu.VMEM((ni, nk, levels), f32),
            pltpu.VMEM((ni, nk, levels), f32),
            pltpu.VMEM((ni, nk, levels), f32),
            dma((2,)),
            dma((10,)),
            dma((STEPS, chunks, 2)),
            dma((STEPS, 2)),
            dma((STEPS, chunks, 2)),
            dma((ni // min(PIECE, rows),)),
            dma((CHAIN,)),
            dma((CHAIN,)),
            pltpu.SemaphoreType.REGULAR,
        ],
        compiler_params=pltpu.CompilerParams(
            collective_id=0, has_side_effects=True, vmem_limit_bytes=48 * 2**20),
        name="march",
    )(tracer, crowding)


def sums_kernel(scale, block, end, carried, sums, copied, held, sem):
    nj, ni = end.shape[:2]
    blocks = ni // block

    def written(n, b):
        at_b = pl.ds(b * block, block)
        source, target = ((end, copied), (held, sums))[n]
        return pltpu.make_async_copy(source.at[:, at_b], target.at[:, at_b], sem.at[n, b])

    for b in range(blocks):
        written(0, b).start()
    for b in range(blocks):
        @pl.loop(b * block, (b + 1) * block)
        def _(i):
            run = carried[i]
            for j in range(nj):
                run = run + end[j, i]
                held[j, i] = run * scale
        written(1, b).start()
    for b in range(blocks):
        for n in (0, 1):
            written(n, b).wait()


def sums_along_j(end, carried, cells):
    ni = end.shape[1]
    block = min(8, ni)
    return pl.pallas_call(
        functools.partial(sums_kernel, 1.0 / cells, block),
        out_shape=(jax.ShapeDtypeStruct(end.shape, end.dtype),) * 2,
        in_specs=[pl.BlockSpec(memory_space=pltpu.VMEM)] * 2,
        out_specs=(pl.BlockSpec(memory_space=pl.ANY),) * 2,
        scratch_shapes=[pltpu.VMEM(end.shape, end.dtype), pltpu.SemaphoreType.DMA((2, ni // block))],
        compiler_params=pltpu.CompilerParams(vmem_limit_bytes=12 * 2**20),
        name="sums",
    )(end, carried)


def on_device(tracer, crowding):
    end, carried = march(tracer, crowding, min(ROWS, tracer.shape[1] // 2))
    return sums_along_j(end, carried, tracer.shape[0] * lax.axis_size("lat"))


def solution(mesh):
    spec = P(("unit", "lat"), "lon", "lev", None)
    return jax.shard_map(
        on_device, mesh=mesh, in_specs=(spec, spec), out_specs=(spec, spec), check_vma=False)
```
